128 devices in a mesh: blk: 8 (over y, x_lo), inner: 16 (over z, x_hi, core).
Axes of the slice: x: 4 (x_hi: 2, x_lo: 2; x = x_hi * 2 + x_lo), y: 4, z: 4, core: 2. Of those that a mesh axis runs over, the one named last changes fastest.
Arguments:
- points: float32 [16384, 128], P(('blk', 'inner')), may hold values from -8 to 8
- lengthscales: float32 [128], replicated, may hold values from 6 to 24
- noise_level: float32 [1], replicated, may hold values from 1 to 10
- iterate: float32 [16384, 64], P(('blk', 'inner')), may hold values from -6 to 6
- residual: float32 [16384, 64], P(('blk', 'inner')), may hold values from -6 to 6
- direction: float32 [16384, 64], P(('blk', 'inner')), may hold values from -6 to 6
Outputs:
- new_iterate: float32 [16384, 64], P(('blk', 'inner'))
- new_residual: float32 [16384, 64], P(('blk', 'inner'))
- new_direction: float32 [16384, 64], P(('blk', 'inner'))
The draws below stay inside these ranges and needn't reach their ends.
All inputs are finite; a program needn't handle non-finite values.
Results may differ from the reference program's by a relative error of at most 0.00014.
Values sent between devices are 32-bit elements; how exact they have to be, the bound alone decides.
No kernel may reach another device: no remote copies, remote signals or barrier semaphores. Data moves between devices by JAX's collectives and lax.ppermute only.
A program may use at most 64 MiB of HBM per device.

```python
import math
import jax
import jax.numpy as jnp
from jax import lax

D = 128
RHS = 64
PTS_DEV = 128
NPTS = 16384


def draw_points(key, part):
    clusters = max(NPTS // 128, 4)
    key_member = jax.random.fold_in(key, 101)
    key_centre = jax.random.fold_in(key, 202)
    key_spread = jax.random.fold_in(key, 404)
    member = jax.random.randint(key_member, (NPTS,), 0, clusters)
    centres = 2.0 * jax.random.normal(key_centre, (clusters, D), jnp.float32)
    spread = jax.random.normal(key_spread, (NPTS, D), jnp.float32)
    values = centres[member] + spread
    return jnp.clip(values, -8.0, 8.0).astype(jnp.float32)


def block_scale(own_key, shape, pieces, smallest, top_value):
    def one(position, blocks):
        draws = jax.random.uniform(jax.random.fold_in(jax.random.fold_in(own_key, 6), position), (blocks,), jnp.float32, smallest / len(pieces), top_value / len(pieces))
        return jnp.repeat(jnp.exp(draws), shape[position] // blocks).reshape((-1,) + (1,) * (len(shape) - position - 1))

    gain = one(*pieces[0])
    for cut in pieces[1:]:
        gain = gain * one(*cut)
    return gain


def noise(stream_key, extent, scale, limit, pieces=(), dtype=jnp.bfloat16):
    array = jax.random.normal(stream_key, extent, jnp.float32) * scale
    if len(pieces) > 0:
        array = block_scale(stream_key, extent, pieces, -0.22, 0.18) * array
    return jnp.clip(array, min=-limit, max=limit).astype(dtype)


def setup_inputs(seed: int = 0) -> dict:
    seeds = jax.random.split(jax.random.key(seed), 7)
    points = draw_points(jax.random.fold_in(seeds[6], 71), 0)
    lengthscales = jnp.clip(jnp.exp(jax.random.uniform(seeds[1], (D,), jnp.float32, math.log(6.0), math.log(24.0))), 6.0, 24.0)
    noise_level = jnp.clip(jnp.exp(jax.random.uniform(seeds[2], (1,), jnp.float32, math.log(1.0), math.log(10.0))), 1.0, 10.0)
    iterate = noise(seeds[3], (NPTS, RHS), 1.0, 6.0, ((0, 128),), jnp.float32)
    residual = noise(seeds[4], (NPTS, RHS), 1.0, 6.0, ((0, 128),), jnp.float32)
    direction = noise(seeds[5], (NPTS, RHS), 1.0, 6.0, ((0, 128),), jnp.float32)
    return dict(points=points, lengthscales=lengthscales, noise_level=noise_level, iterate=iterate, residual=residual, direction=direction)


def kernel_block(left, left_sq, right, right_sq):
    products = lax.dot_general(left.astype(jnp.float32), right.astype(jnp.float32), (((1,), (1,)), ((), ())), precision=lax.Precision.HIGHEST, preferred_element_type=jnp.float32)
    return jnp.exp(-0.5 * (left_sq[:, None] + right_sq[None, :] - 2.0 * products))

def matmul(left, right):
    return jnp.dot(left.astype(jnp.float32), right.astype(jnp.float32), precision=lax.Precision.HIGHEST, preferred_element_type=jnp.float32)

def transposed(left, right):
    return lax.dot_general(left.astype(jnp.float32), right.astype(jnp.float32), (((0,), (0,)), ((), ())), precision=lax.Precision.HIGHEST, preferred_element_type=jnp.float32)

def chol_solve(matrix, rhs_side):
    factor = jnp.linalg.cholesky(matrix)
    return jax.scipy.linalg.cho_solve((factor, True), rhs_side)

def reference(points, lengthscales, noise_level, iterate, residual, direction):
    scaled = points / lengthscales[None, :]
    sq_norms = jnp.sum(scaled * scaled, axis=1)
    blocks = scaled.reshape(NPTS // PTS_DEV, PTS_DEV, D)
    block_sq = sq_norms.reshape(NPTS // PTS_DEV, PTS_DEV)

    def one_block(pair):
        rows, rows_sq = pair
        return matmul(kernel_block(rows, rows_sq, scaled, sq_norms), direction)
    image = lax.map(one_block, (blocks, block_sq)).reshape(NPTS, RHS)
    image = image + noise_level[0] * direction
    gram_raw = transposed(direction, image)
    gram_matrix = 0.5 * (gram_raw + gram_raw.T)
    res_gram = transposed(residual, residual)
    step_size = chol_solve(gram_matrix, res_gram)
    new_iterate = iterate + matmul(direction, step_size)
    new_residual = residual - matmul(image, step_size)
    new_gram = transposed(new_residual, new_residual)
    correction = chol_solve(res_gram, new_gram)
    new_direction = new_residual + matmul(direction, correction)
    return (new_iterate, new_residual, new_direction)
```

```python
import functools
import math

import jax
import jax.numpy as jnp
from jax import lax
from jax.experimental import pallas as pl
from jax.experimental.pallas import tpu as pltpu
from jax.sharding import Mesh, PartitionSpec as P

AXES = ("y", "xl", "z", "xh", "core")
BLK = ("y", "xl")
CHIPS = ("z", "xh")
N = 128
F = 128
Q = 64
G = 8
HI = lax.Precision.HIGHEST
ROOT = math.sqrt(math.log2(math.e))
VM = pl.BlockSpec(memory_space=pltpu.VMEM)


def call(body, outs, scratch=(), flops=10**6):
    return pl.pallas_call(
        body,
        out_shape=outs,
        out_specs=jax.tree.map(lambda _: VM, outs),
        scratch_shapes=list(scratch),
        cost_estimate=pl.CostEstimate(flops=flops, bytes_accessed=10**6, transcendentals=0),
    )


def f32(*shape):
    return jax.ShapeDtypeStruct(shape, jnp.float32)


def dot(a, b, ca=1, cb=0, precision=HI):
    return lax.dot_general(
        a, b, (((ca,), (cb,)), ((), ())), precision=precision, preferred_element_type=jnp.float32
    )


def low_lanes(shape):
    return lax.broadcasted_iota(jnp.int32, shape, 1) < Q


def fold(wide):
    half = wide.shape[0] // 2
    return jnp.where(low_lanes((half, 128)), wide[:half], wide[half:])


def unfold(packed):
    return jnp.concatenate([packed[:, :Q], packed[:, Q:]], axis=0)


def prep(points, scales, direction, residual, rows, cols):
    unit = points[...] / scales[...] * ROOT
    half = 0.5 * jnp.sum(unit * unit, axis=1, keepdims=True)
    as_row = jnp.broadcast_to(half, (N, N)).T[:8]
    gram = dot(residual[...], residual[...], 0, 0)
    for i in range(G):
        rows[i] = unit
        cols[i, :N, :F] = unit
        cols[i, :N, F : F + Q] = direction[...]
        cols[i, :Q, F + Q :] = gram
        cols[i, N:, :F] = as_row


def split(value):
    top = value.astype(jnp.bfloat16)
    rest = value - top.astype(jnp.float32)
    mid = rest.astype(jnp.bfloat16)
    low = (rest - mid.astype(jnp.float32)).astype(jnp.bfloat16)
    return top, mid, low


def products(first, tile, rows, cols, *refs):
    before, out, right, dirs, halves, left = refs if not first else (None, *refs)
    for j in range(G):
        at = slice(j * N, (j + 1) * N)
        top, mid, low = split(cols[j, :N, :F])
        right[at] = jnp.concatenate([top, mid, top, low, top, mid], axis=1)
        high, rest, _ = split(cols[j, :N, F : F + Q])
        dirs[at] = jnp.concatenate([high, rest], axis=1)
        halves[:, at] = cols[j, N:, :F]
    per = tile // N

    def step(i, carry):
        unit = rows[pl.ds(i * per, per)].reshape(tile, F)
        top, mid, low = split(unit)
        left[...] = jnp.concatenate([top, top, mid, top, low, mid], axis=1)
        half = 0.5 * jnp.sum(unit * unit, axis=1, keepdims=True)
        total = jnp.zeros((tile, 2 * Q), jnp.float32)
        for j in range(4):
            at = slice(j * 256, (j + 1) * 256)
            inner = dot(left[...], right[at], 1, 1, None)
            kernel = jnp.exp2(inner - half - halves[0:1, at])
            high = kernel.astype(jnp.bfloat16)
            rest = (kernel - high.astype(jnp.float32)).astype(jnp.bfloat16)
            total += dot(high, dirs[at], 1, 0, None) + dot(rest, dirs[at], 1, 0, None)
        if first:
            out[pl.ds(i * tile, tile)] = total
        else:
            total += before[pl.ds(i * tile, tile)]
            total += pltpu.roll(total, Q, 1)
            for b in range(per):
                out[i * per + b, :Q] = fold(total[b * N : (b + 1) * N])
        return carry

    lax.fori_loop(0, (G * N) // tile, step, 0)


def products_first(tile, rows, cols, *refs):
    products(True, tile, rows, cols, *refs)


def products_last(tile, rows, cols, mine, before, out, right, dirs, halves, left):
    products(False, tile, rows, cols, before, out, right, dirs, halves, left)
    gram = cols[0, :Q, F + Q :] + mine[0, :Q, F + Q :]
    for j in range(1, G):
        gram += cols[j, :Q, F + Q :] + mine[j, :Q, F + Q :]
    packed = fold(jnp.concatenate([gram, gram], axis=1))
    for j in range(G):
        out[j, Q:] = packed


def summed(pieces):
    total = pieces[0]
    for j in range(1, G):
        total += pieces[j]
    return total


def grams(pieces, noise, direction, residual, image_out, gram_out, sums):
    total = summed(pieces)
    image = unfold(total[:Q]) + noise[0, 0] * direction[...]
    image_out[...] = image
    gram_out[...] = unfold(total[Q:])
    side = jnp.concatenate([direction[...], residual[...]], axis=1)
    sums[:Q] = dot(image, side, 0, 0)
    square = dot(image, image, 0, 0)
    sums[Q:] = fold(jnp.concatenate([square, square], axis=1))


def eliminate(matrix):
    slabs = [matrix[8 * r : 8 * r + 8] for r in range(8)]
    sub = lax.broadcasted_iota(jnp.int32, (8, 128), 0)
    for k in range(8):
        spread = [
            [jnp.broadcast_to(slabs[r][:, 8 * k + j : 8 * k + j + 1], (8, 128)) for j in range(8)]
            for r in range(8)
        ]
        own, pivot = spread[k], slabs[k]
        for j in range(8):
            inverse = 1.0 / jnp.broadcast_to(own[j][j : j + 1], (8, 128))
            at = sub == j

            def cleared(value):
                row = jnp.broadcast_to(value[j : j + 1], (8, 128)) * inverse
                return jnp.where(at, row, value - own[j] * row)

            pivot = cleared(pivot)
            own = own[: j + 1] + [cleared(c) for c in own[j + 1 :]]
        for r in range(8):
            if r != k:
                for j in range(8):
                    slabs[r] = slabs[r] - spread[r][j] * jnp.broadcast_to(
                        pivot[j : j + 1], (8, 128)
                    )
        slabs[k] = pivot
    return jnp.concatenate(slabs, axis=0)[:, Q:]


def invert(gram, out):
    eye = lax.broadcasted_iota(jnp.int32, (Q, Q), 0) == lax.broadcasted_iota(jnp.int32, (Q, Q), 1)
    out[...] = eliminate(jnp.concatenate([gram[...], eye.astype(jnp.float32)], axis=1))


def pair_sum(a, b, out):
    total = a[...] + b[...]
    for j in range(G):
        out[j] = total


def chip_sum(pieces, out):
    total = summed(pieces)
    for j in range(G):
        out[j] = total


def finish(pieces, gram, inverse, image, iterate, residual, direction, x_out, r_out, d_out):
    total = summed(pieces)
    raw, cross = total[:Q, :Q], total[:Q, Q:]
    square = unfold(total[Q:])
    res = gram[...]
    step = eliminate(jnp.concatenate([0.5 * (raw + raw.T), res], axis=1))
    x_out[...] = iterate[...] + dot(direction[...], step)
    new_res = residual[...] - dot(image[...], step)
    r_out[...] = new_res
    term = dot(step, cross, 0, 0)
    new_gram = res - term - term.T + dot(step, dot(square, step), 0, 0)
    d_out[...] = new_res + dot(direction[...], dot(inverse[...], new_gram))


def swapped(value):
    return lax.ppermute(value, "core", [(0, 1), (1, 0)])


def exchanged(value, axes):
    return lax.all_to_all(value, axes, 0, 0, tiled=True)


def on_device(points, lengthscales, noise_level, iterate, residual, direction):
    rows, cols = call(prep, [f32(G, N, F), f32(G, N + 8, 256)])(
        points, lengthscales.reshape(1, F), direction, residual
    )
    cols = exchanged(cols, BLK)
    rows = exchanged(rows, CHIPS)
    other = swapped(cols)
    tile = 512
    scratch = [
        pltpu.VMEM((G * N, 6 * F), jnp.bfloat16),
        pltpu.VMEM((G * N, 2 * Q), jnp.bfloat16),
        pltpu.VMEM((8, G * N), jnp.float32),
        pltpu.VMEM((tile, 6 * F), jnp.bfloat16),
    ]
    part = call(
        functools.partial(products_first, tile), f32(G * N, 2 * Q), scratch, flops=4 * 10**9
    )(rows, cols)
    sent = call(
        functools.partial(products_last, tile), f32(G, Q + Q // 2, 128), scratch, flops=4 * 10**9
    )(rows, other, cols, part)
    pieces = exchanged(sent, CHIPS)
    image, gram, sums = call(grams, [f32(N, Q), f32(Q, Q), f32(Q + Q // 2, 128)])(
        pieces, noise_level.reshape(1, 1), direction, residual
    )
    both = call(pair_sum, f32(G, Q + Q // 2, 128))(sums, swapped(sums))
    inverse = call(invert, f32(Q, Q), flops=10**8)(gram)
    by_chip = call(chip_sum, f32(G, Q + Q // 2, 128))(exchanged(both, CHIPS))
    whole = exchanged(by_chip, BLK)
    return tuple(
        call(finish, [f32(N, Q)] * 3)(whole, gram, inverse, image, iterate, residual, direction)
    )


def solution(mesh):
    fine = Mesh(mesh.devices.reshape(4, 2, 4, 2, 2), AXES)
    split_rows = P(AXES, None)
    return jax.shard_map(
        on_device,
        mesh=fine,
        in_specs=(split_rows, P(), P(), split_rows, split_rows, split_rows),
        out_specs=(split_rows,) * 3,
        check_vma=False,
    )
```

```python
import functools
import math

import jax
import jax.numpy as jnp
from jax import lax
from jax.experimental import pallas as pl
from jax.experimental.pallas import tpu as pltpu
from jax.sharding import Mesh, PartitionSpec as P

AXES = ("y", "xl", "z", "xh", "core")
BLK = ("y", "xl")
CHIPS = ("z", "xh")
N = 128
F = 128
Q = 64
G = 8
HI = lax.Precision.HIGHEST
ROOT = math.sqrt(math.log2(math.e))
DIRS = N + Q
GRAM = DIRS + Q // 2
ROWS = GRAM + 8
VM = pl.BlockSpec(memory_space=pltpu.VMEM)


def call(body, outs, scratch=(), flops=10**6, room=4):
    return pl.pallas_call(
        body,
        out_shape=outs,
        out_specs=jax.tree.map(lambda _: VM, outs),
        scratch_shapes=list(scratch),
        compiler_params=pltpu.CompilerParams(vmem_limit_bytes=room * 2**20),
        cost_estimate=pl.CostEstimate(flops=flops, bytes_accessed=10**6, transcendentals=0),
    )


def f32(*shape):
    return jax.ShapeDtypeStruct(shape, jnp.float32)


def dot(a, b, ca=1, cb=0, precision=HI):
    return lax.dot_general(
        a, b, (((ca,), (cb,)), ((), ())), precision=precision, preferred_element_type=jnp.float32
    )


def low_lanes(shape):
    return lax.broadcasted_iota(jnp.int32, shape, 1) < Q


def fold(wide):
    half = wide.shape[0] // 2
    return jnp.where(low_lanes((half, 128)), wide[:half], wide[half:])


def unfold(packed):
    return jnp.concatenate([packed[:, :Q], packed[:, Q:]], axis=0)


def prep(points, scales, direction, residual, rows, cols):
    unit = points[...] / scales[...] * ROOT
    half = 0.5 * jnp.sum(unit * unit, axis=1, keepdims=True)
    as_row = jnp.broadcast_to(half, (N, N)).T[:8]
    twice = jnp.concatenate([residual[...], residual[...]], axis=0)
    gram = fold(dot(residual[...], twice, 1, 1))
    for i in range(G):
        rows[i] = unit
        cols[i, :N] = unit
        cols[i, N:DIRS] = direction[...]
        cols[i, DIRS:GRAM] = gram
        cols[i, GRAM:] = as_row


def split(value):
    top = value.astype(jnp.bfloat16)
    rest = value - top.astype(jnp.float32)
    mid = rest.astype(jnp.bfloat16)
    low = (rest - mid.astype(jnp.float32)).astype(jnp.bfloat16)
    return top, mid, low


def products(first, tile, rows, cols, *refs):
    before, out, right, dirs, halves, left = refs if not first else (None, *refs)
    for j in range(G):
        at = slice(j * N, (j + 1) * N)
        top, mid, low = split(cols[j, :N])
        right[at] = jnp.concatenate([top, mid, top, low, top, mid], axis=1)
        high, rest, _ = split(cols[j, N:DIRS])
        dirs[:, at] = jnp.concatenate([high, rest], axis=0)
        halves[:, at] = cols[j, GRAM:]
    per = tile // N

    def step(i, carry):
        unit = rows[pl.ds(i * per, per)].reshape(tile, F)
        top, mid, low = split(unit)
        left[...] = jnp.concatenate([top, top, mid, top, low, mid], axis=1)
        half = 0.5 * jnp.sum(unit * unit, axis=1, keepdims=True)
        total = jnp.zeros((tile, 2 * Q), jnp.float32)
        for j in range(4):
            at = slice(j * 256, (j + 1) * 256)
            inner = dot(left[...], right[at], 1, 1, None)
            kernel = jnp.exp2(inner - half - halves[0:1, at])
            high = kernel.astype(jnp.bfloat16)
            rest = (kernel - high.astype(jnp.float32)).astype(jnp.bfloat16)
            total += dot(high, dirs[:, at], 1, 1, None) + dot(rest, dirs[:, at], 1, 1, None)
        if first:
            out[pl.ds(i * tile, tile)] = total
        else:
            total += before[pl.ds(i * tile, tile)]
            total += pltpu.roll(total, Q, 1)
            for b in range(per):
                out[i * per + b, :Q] = fold(total[b * N : (b + 1) * N])
        return carry

    lax.fori_loop(0, (G * N) // tile, step, 0)


def products_first(tile, rows, cols, *refs):
    products(True, tile, rows, cols, *refs)


def products_last(tile, rows, cols, mine, before, out, right, dirs, halves, left):
    products(False, tile, rows, cols, before, out, right, dirs, halves, left)
    gram = cols[0, DIRS:GRAM] + mine[0, DIRS:GRAM]
    for j in range(1, G):
        gram += cols[j, DIRS:GRAM] + mine[j, DIRS:GRAM]
    for j in range(G):
        out[j, Q:] = gram


def summed(pieces):
    total = pieces[0]
    for j in range(1, G):
        total += pieces[j]
    return total


def grams(pieces, noise, direction, residual, image_out, gram_out, sums):
    total = summed(pieces)
    turned = total[:Q].T
    image = jnp.concatenate([turned[:Q], turned[Q:]], axis=1) + noise[0, 0] * direction[...]
    image_out[...] = image
    gram_out[...] = unfold(total[Q:])
    side = jnp.concatenate([direction[...], residual[...], image, image], axis=0)
    products_of = dot(image, side, 1, 1)
    sums[:Q] = products_of[:, : 2 * Q]
    sums[Q:] = fold(products_of[:, 2 * Q :])


def eliminate(matrix):
    slabs = [matrix[8 * r : 8 * r + 8] for r in range(8)]
    sub = lax.broadcasted_iota(jnp.int32, (8, 128), 0)
    for k in range(8):
        spread = [
            [jnp.broadcast_to(slabs[r][:, 8 * k + j : 8 * k + j + 1], (8, 128)) for j in range(8)]
            for r in range(8)
        ]
        own, pivot = spread[k], slabs[k]
        for j in range(8):
            inverse = 1.0 / jnp.broadcast_to(own[j][j : j + 1], (8, 128))
            at = sub == j

            def cleared(value):
                row = jnp.broadcast_to(value[j : j + 1], (8, 128)) * inverse
                return jnp.where(at, row, value - own[j] * row)

            pivot = cleared(pivot)
            own = own[: j + 1] + [cleared(c) for c in own[j + 1 :]]
        for r in range(8):
            if r != k:
                for j in range(8):
                    slabs[r] = slabs[r] - spread[r][j] * jnp.broadcast_to(
                        pivot[j : j + 1], (8, 128)
                    )
        slabs[k] = pivot
    return jnp.concatenate(slabs, axis=0)[:, Q:]


def invert(gram, out):
    eye = lax.broadcasted_iota(jnp.int32, (Q, Q), 0) == lax.broadcasted_iota(jnp.int32, (Q, Q), 1)
    out[...] = eliminate(jnp.concatenate([gram[...], eye.astype(jnp.float32)], axis=1))


def pair_sum(a, b, out):
    total = a[...] + b[...]
    for j in range(G):
        out[j] = total


def chip_sum(pieces, out):
    total = summed(pieces)
    for j in range(G):
        out[j] = total


def finish(pieces, gram, inverse, image, iterate, residual, direction, x_out, r_out, d_out):
    total = summed(pieces)
    raw, cross = total[:Q, :Q], total[:Q, Q:]
    square = unfold(total[Q:])
    res = gram[...]
    step = eliminate(jnp.concatenate([0.5 * (raw + raw.T), res], axis=1))
    x_out[...] = iterate[...] + dot(step, direction[...], 0, 0)
    new_res = residual[...] - dot(step, image[...], 0, 0)
    r_out[...] = new_res
    term = dot(step, cross, 0, 0)
    new_gram = res - term - term.T + dot(step, dot(square, step), 0, 0)
    d_out[...] = new_res + dot(dot(inverse[...], new_gram), direction[...], 0, 0)


def swapped(value):
    return lax.ppermute(value, "core", [(0, 1), (1, 0)])


def exchanged(value, axes):
    return lax.all_to_all(value, axes, 0, 0, tiled=True)


def on_device(points, lengthscales, noise_level, iterate, residual, direction):
    iterate, residual, direction = iterate.T, residual.T, direction.T
    rows, cols = call(prep, [f32(G, N, F), f32(G, ROWS, 128)])(
        points, lengthscales.reshape(1, F), direction, residual
    )
    cols = exchanged(cols, BLK)
    rows = exchanged(rows, CHIPS)
    other = swapped(cols)
    tile = 512
    scratch = [
        pltpu.VMEM((G * N, 6 * F), jnp.bfloat16),
        pltpu.VMEM((2 * Q, G * N), jnp.bfloat16),
        pltpu.VMEM((8, G * N), jnp.float32),
        pltpu.VMEM((tile, 6 * F), jnp.bfloat16),
    ]
    part = call(
        functools.partial(products_first, tile), f32(G * N, 2 * Q), scratch, 4 * 10**9, 16
    )(rows, cols)
    sent = call(
        functools.partial(products_last, tile), f32(G, Q + Q // 2, 128), scratch, 4 * 10**9, 16
    )(rows, other, cols, part)
    pieces = exchanged(sent, CHIPS)
    image, gram, sums = call(grams, [f32(Q, N), f32(Q, Q), f32(Q + Q // 2, 128)])(
        pieces, noise_level.reshape(1, 1), direction, residual
    )
    both = call(pair_sum, f32(G, Q + Q // 2, 128))(sums, swapped(sums))
    inverse = call(invert, f32(Q, Q), flops=10**8)(gram)
    by_chip = call(chip_sum, f32(G, Q + Q // 2, 128))(exchanged(both, CHIPS))
    whole = exchanged(by_chip, BLK)
    outs = call(finish, [f32(Q, N)] * 3)(
        whole, gram, inverse, image, iterate, residual, direction
    )
    return tuple(o.T for o in outs)


def solution(mesh):
    fine = Mesh(mesh.devices.reshape(4, 2, 4, 2, 2), AXES)
    split_rows = P(AXES, None)
    return jax.shard_map(
        on_device,
        mesh=fine,
        in_specs=(split_rows, P(), P(), split_rows, split_rows, split_rows),
        out_specs=(split_rows,) * 3,
        check_vma=False,
    )
```

```python
import math

import jax
import jax.numpy as jnp
from jax import lax
from jax.experimental import pallas as pl
from jax.experimental.pallas import tpu as pltpu
from jax.sharding import Mesh, PartitionSpec as P

AXES = ("y", "xl", "z", "xh", "core")
BLK = ("y", "xl")
CHIPS = ("z", "xh")
PLANE = ("y", "xl", "xh")
N = 128
F = 128
Q = 64
G = 8
R = 16
C = 8
TILE = 512
CHUNK = 256
HI = lax.Precision.HIGHEST
ROOT = math.sqrt(math.log2(math.e))
DIRS = N + Q
GRAM = DIRS + Q // 2
ROWS = GRAM + 8
VM = pl.BlockSpec(memory_space=pltpu.VMEM)


def call(body, outs, scratch=(), flops=10**6, room=4):
    return pl.pallas_call(
        body,
        out_shape=outs,
        out_specs=jax.tree.map(lambda _: VM, outs),
        scratch_shapes=list(scratch),
        compiler_params=pltpu.CompilerParams(vmem_limit_bytes=room * 2**20),
        cost_estimate=pl.CostEstimate(flops=flops, bytes_accessed=10**6, transcendentals=0),
    )


def f32(*shape):
    return jax.ShapeDtypeStruct(shape, jnp.float32)


def dot(a, b, ca=1, cb=0, precision=HI):
    return lax.dot_general(
        a, b, (((ca,), (cb,)), ((), ())), precision=precision, preferred_element_type=jnp.float32
    )


def low_lanes(shape):
    return lax.broadcasted_iota(jnp.int32, shape, 1) < Q


def fold(wide):
    half = wide.shape[0] // 2
    return jnp.where(low_lanes((half, 128)), wide[:half], wide[half:])


def unfold(packed):
    return jnp.concatenate([packed[:, :Q], packed[:, Q:]], axis=0)


def prep(points, scales, direction, residual, rows, cols):
    unit = points[...] / scales[...] * ROOT
    half = 0.5 * jnp.sum(unit * unit, axis=1, keepdims=True)
    twice = jnp.concatenate([residual[...], residual[...]], axis=0)
    for i in range(R):
        rows[i] = unit
    cols[:N] = unit
    cols[N:DIRS] = direction[...]
    cols[DIRS:GRAM] = fold(dot(residual[...], twice, 1, 1))
    cols[GRAM:] = jnp.broadcast_to(half, (N, N)).T[:8]


def split(value):
    top = value.astype(jnp.bfloat16)
    rest = value - top.astype(jnp.float32)
    mid = rest.astype(jnp.bfloat16)
    low = (rest - mid.astype(jnp.float32)).astype(jnp.bfloat16)
    return top, mid, low


def spread_cols(*refs):
    cols, (right, dirs, halves, gram) = refs[:C], refs[C:]
    total = cols[0][DIRS:GRAM]
    for j in range(C):
        at = slice(j * N, (j + 1) * N)
        top, mid, low = split(cols[j][:N])
        right[at] = jnp.concatenate([top, mid, top, low, top, mid], axis=1)
        high, rest, _ = split(cols[j][N:DIRS])
        dirs[:, at] = jnp.concatenate([high, rest], axis=0)
        halves[:, at] = cols[j][GRAM:]
        if j > 0:
            total += cols[j][DIRS:GRAM]
    gram[...] = total


def products(rows, right, dirs, halves, gram, out, left):
    per = TILE // N

    def step(i, carry):
        unit = rows[pl.ds(i * per, per)].reshape(TILE, F)
        top, mid, low = split(unit)
        left[...] = jnp.concatenate([top, top, mid, top, low, mid], axis=1)
        half = 0.5 * jnp.sum(unit * unit, axis=1, keepdims=True)
        total = jnp.zeros((TILE, 2 * Q), jnp.float32)
        for j in range(C * N // CHUNK):
            at = slice(j * CHUNK, (j + 1) * CHUNK)
            inner = dot(left[...], right[at], 1, 1, None)
            kernel = jnp.exp2(inner - half - halves[0:1, at])
            high = kernel.astype(jnp.bfloat16)
            rest = (kernel - high.astype(jnp.float32)).astype(jnp.bfloat16)
            total += dot(high, dirs[:, at], 1, 1, None) + dot(rest, dirs[:, at], 1, 1, None)
        total += pltpu.roll(total, Q, 1)
        for b in range(per):
            out[i * per + b, :Q] = fold(total[b * N : (b + 1) * N])
            out[i * per + b, Q:] = gram[...]
        return carry

    lax.fori_loop(0, R // per, step, 0)


def summed(pieces):
    total = pieces[0]
    for j in range(1, pieces.shape[0]):
        total += pieces[j]
    return total


def grams(pieces, noise, direction, residual, image_out, gram_out, sums):
    total = summed(pieces)
    turned = total[:Q].T
    image = jnp.concatenate([turned[:Q], turned[Q:]], axis=1) + noise[0, 0] * direction[...]
    image_out[...] = image
    gram_out[...] = unfold(total[Q:])
    side = jnp.concatenate([direction[...], residual[...], image, image], axis=0)
    products_of = dot(image, side, 1, 1)
    sums[:Q] = products_of[:, : 2 * Q]
    sums[Q:] = fold(products_of[:, 2 * Q :])


def eliminate(matrix):
    slabs = [matrix[8 * r : 8 * r + 8] for r in range(8)]
    sub = lax.broadcasted_iota(jnp.int32, (8, 128), 0)
    for k in range(8):
        spread = [
            [jnp.broadcast_to(slabs[r][:, 8 * k + j : 8 * k + j + 1], (8, 128)) for j in range(8)]
            for r in range(8)
        ]
        own, pivot = spread[k], slabs[k]
        for j in range(8):
            inverse = 1.0 / jnp.broadcast_to(own[j][j : j + 1], (8, 128))
            at = sub == j

            def cleared(value):
                row = jnp.broadcast_to(value[j : j + 1], (8, 128)) * inverse
                return jnp.where(at, row, value - own[j] * row)

            pivot = cleared(pivot)
            own = own[: j + 1] + [cleared(c) for c in own[j + 1 :]]
        for r in range(8):
            if r != k:
                for j in range(8):
                    slabs[r] = slabs[r] - spread[r][j] * jnp.broadcast_to(
                        pivot[j : j + 1], (8, 128)
                    )
        slabs[k] = pivot
    return jnp.concatenate(slabs, axis=0)[:, Q:]


def invert(gram, out):
    eye = lax.broadcasted_iota(jnp.int32, (Q, Q), 0) == lax.broadcasted_iota(jnp.int32, (Q, Q), 1)
    out[...] = eliminate(jnp.concatenate([gram[...], eye.astype(jnp.float32)], axis=1))


def pair_sum(a, b, out):
    total = a[...] + b[...]
    for j in range(G):
        out[j] = total


def chip_sum(pieces, out):
    total = summed(pieces)
    for j in range(G):
        out[j] = total


def finish(pieces, gram, inverse, image, iterate, residual, direction, x_out, r_out, d_out):
    total = summed(pieces)
    raw, cross = total[:Q, :Q], total[:Q, Q:]
    square = unfold(total[Q:])
    res = gram[...]
    step = eliminate(jnp.concatenate([0.5 * (raw + raw.T), res], axis=1))
    x_out[...] = iterate[...] + dot(step, direction[...], 0, 0)
    new_res = residual[...] - dot(step, image[...], 0, 0)
    r_out[...] = new_res
    term = dot(step, cross, 0, 0)
    new_gram = res - term - term.T + dot(step, dot(square, step), 0, 0)
    d_out[...] = new_res + dot(dot(inverse[...], new_gram), direction[...], 0, 0)


def swapped(value):
    return lax.ppermute(value, "core", [(0, 1), (1, 0)])


def across(value, k):
    return lax.ppermute(value, "z", [(i, i ^ k) for i in range(4)])


def exchanged(value, axes):
    return lax.all_to_all(value, axes, 0, 0, tiled=True)


def on_device(points, lengthscales, noise_level, iterate, residual, direction):
    iterate, residual, direction = iterate.T, residual.T, direction.T
    rows, own = call(prep, [f32(R, N, F), f32(ROWS, 128)])(
        points, lengthscales.reshape(1, F), direction, residual
    )
    rows = exchanged(rows, PLANE)
    mine = [own] + [across(own, k) for k in range(1, 4)]
    cols = mine + [swapped(m) for m in mine]
    spread = call(
        spread_cols,
        [
            jax.ShapeDtypeStruct((C * N, 6 * F), jnp.bfloat16),
            jax.ShapeDtypeStruct((2 * Q, C * N), jnp.bfloat16),
            f32(8, C * N),
            f32(Q // 2, 128),
        ],
        flops=10**8,
    )(*cols)
    sent = call(
        products,
        f32(R, Q + Q // 2, 128),
        [pltpu.VMEM((TILE, 6 * F), jnp.bfloat16)],
        8 * 10**9,
        24,
    )(rows, *spread)
    pieces = exchanged(sent, PLANE)
    image, gram, sums = call(grams, [f32(Q, N), f32(Q, Q), f32(Q + Q // 2, 128)])(
        pieces, noise_level.reshape(1, 1), direction, residual
    )
    both = call(pair_sum, f32(G, Q + Q // 2, 128))(sums, swapped(sums))
    inverse = call(invert, f32(Q, Q), flops=10**8)(gram)
    by_chip = call(chip_sum, f32(G, Q + Q // 2, 128))(exchanged(both, CHIPS))
    whole = exchanged(by_chip, BLK)
    outs = call(finish, [f32(Q, N)] * 3)(
        whole, gram, inverse, image, iterate, residual, direction
    )
    return tuple(o.T for o in outs)


def solution(mesh):
    fine = Mesh(mesh.devices.reshape(4, 2, 4, 2, 2), AXES)
    split_rows = P(AXES, None)
    return jax.shard_map(
        on_device,
        mesh=fine,
        in_specs=(split_rows, P(), P(), split_rows, split_rows, split_rows),
        out_specs=(split_rows,) * 3,
        check_vma=False,
    )
```

```python
import math

import jax
import jax.numpy as jnp
from jax import lax
from jax.experimental import pallas as pl
from jax.experimental.pallas import tpu as pltpu
from jax.sharding import Mesh, PartitionSpec as P

AXES = ("y", "xl", "z", "xh", "core")
BLK = ("y", "xl")
CHIPS = ("z", "xh")
PLANE = ("y", "xl", "xh")
N = 128
F = 128
Q = 64
G = 8
R = 16
C = 8
TILE = 1024
CHUNK = 256
HI = lax.Precision.HIGHEST
ROOT = math.sqrt(math.log2(math.e))
DIRS = N + Q
GRAM = DIRS + Q // 2
ROWS = GRAM + 8
ITER, RES, DIR, NOISE = 0, Q, 2 * Q, 3 * Q
SUMS = Q + 8
HBM = pl.BlockSpec(memory_space=pltpu.MemorySpace.HBM)
ROOM = 62
VM = pl.BlockSpec(memory_space=pltpu.VMEM)


def call(body, outs, scratch=(), flops=10**6, room=4, ins=None):
    return pl.pallas_call(
        body,
        out_shape=outs,
        **({} if ins is None else {"in_specs": ins}),
        out_specs=jax.tree.map(lambda _: VM, outs),
        scratch_shapes=list(scratch),
        compiler_params=pltpu.CompilerParams(vmem_limit_bytes=room * 2**20),
        cost_estimate=pl.CostEstimate(flops=flops, bytes_accessed=10**6, transcendentals=0),
    )


def f32(*shape):
    return jax.ShapeDtypeStruct(shape, jnp.float32)


def dot(a, b, ca=1, cb=0, precision=HI):
    return lax.dot_general(
        a, b, (((ca,), (cb,)), ((), ())), precision=precision, preferred_element_type=jnp.float32
    )


def low_lanes(shape):
    return lax.broadcasted_iota(jnp.int32, shape, 1) < Q


def fold(wide):
    half = wide.shape[0] // 2
    return jnp.where(low_lanes((half, 128)), wide[:half], wide[half:])


def unfold(packed):
    return jnp.concatenate([packed[:, :Q], packed[:, Q:]], axis=0)


def prep(points, scales, noise, iterate, residual, direction, rows, cols, kept, place, sems):
    points_in, scales_in = place
    copies = [
        pltpu.make_async_copy(points, points_in, sems.at[0]),
        pltpu.make_async_copy(scales, scales_in, sems.at[1]),
        pltpu.make_async_copy(residual, kept.at[RES : RES + Q], sems.at[2]),
        pltpu.make_async_copy(direction, kept.at[DIR : DIR + Q], sems.at[3]),
        pltpu.make_async_copy(iterate, kept.at[ITER : ITER + Q], sems.at[4]),
    ]
    for copy in copies:
        copy.start()
    for copy in copies[:2]:
        copy.wait()
    unit = points_in[...] / scales_in[...] * ROOT
    half = 0.5 * jnp.sum(unit * unit, axis=1, keepdims=True)
    for i in range(R):
        rows[i] = unit
    cols[:N] = unit
    for copy in copies[2:]:
        copy.wait()
    residual = kept[RES : RES + Q]
    cols[N:DIRS] = kept[DIR : DIR + Q]
    cols[DIRS:GRAM] = fold(dot(residual, jnp.concatenate([residual, residual], axis=0), 1, 1))
    cols[GRAM:] = jnp.broadcast_to(half, (N, N)).T[:8]
    kept[NOISE:] = jnp.full((8, 128), noise[0])


def split(value):
    top = value.astype(jnp.bfloat16)
    rest = value - top.astype(jnp.float32)
    mid = rest.astype(jnp.bfloat16)
    low = (rest - mid.astype(jnp.float32)).astype(jnp.bfloat16)
    return top, mid, low


def spread_cols(*refs):
    cols, (right, dirs, halves, gram) = refs[:C], refs[C:]
    total = cols[0][DIRS:GRAM]
    for j in range(C):
        at = slice(j * N, (j + 1) * N)
        top, mid, low = split(cols[j][:N])
        right[at] = jnp.concatenate([top, mid, top, low, top, mid], axis=1)
        high, rest, _ = split(cols[j][N:DIRS])
        dirs[:, at] = jnp.concatenate([high, rest], axis=0)
        halves[:, at] = cols[j][GRAM:]
        if j > 0:
            total += cols[j][DIRS:GRAM]
    gram[...] = total


def products(rows, right, dirs, halves, gram, out, left):
    per = TILE // N

    def step(i, carry):
        unit = rows[pl.ds(i * per, per)].reshape(TILE, F)
        top, mid, low = split(unit)
        left[...] = jnp.concatenate([top, top, mid, top, low, mid], axis=1)
        half = 0.5 * jnp.sum(unit * unit, axis=1, keepdims=True)
        total = jnp.zeros((TILE, 2 * Q), jnp.float32)
        for j in range(C * N // CHUNK):
            at = slice(j * CHUNK, (j + 1) * CHUNK)
            inner = dot(left[...], right[at], 1, 1, None)
            kernel = jnp.exp2(inner - half - halves[0:1, at])
            high = kernel.astype(jnp.bfloat16)
            rest = (kernel - high.astype(jnp.float32)).astype(jnp.bfloat16)
            total += dot(high, dirs[:, at], 1, 1, None) + dot(rest, dirs[:, at], 1, 1, None)
        total += pltpu.roll(total, Q, 1)
        for b in range(per):
            out[i * per + b, :Q] = fold(total[b * N : (b + 1) * N])
            out[i * per + b, Q:] = gram[...]
        return carry

    lax.fori_loop(0, R // per, step, 0)


def summed(pieces):
    total = pieces[0]
    for j in range(1, pieces.shape[0]):
        total += pieces[j]
    return total


def lower(shape):
    return lax.broadcasted_iota(jnp.int32, shape, 0) > lax.broadcasted_iota(jnp.int32, shape, 1)


def diagonal(shape):
    return lax.broadcasted_iota(jnp.int32, shape, 0) == lax.broadcasted_iota(jnp.int32, shape, 1)


def grams(pieces, kept, image_out, gram_out, sums):
    total = summed(pieces)
    turned = total[:Q].T
    direction = kept[DIR : DIR + Q]
    image = jnp.concatenate([turned[:Q], turned[Q:]], axis=1) + kept[NOISE : NOISE + 1] * direction
    image_out[...] = image
    gram_out[...] = unfold(total[Q:])
    side = jnp.concatenate([direction, kept[RES : RES + Q], image], axis=0)
    wide = dot(image, side, 1, 1)
    gram = 0.5 * (wide[:, :Q] + dot(direction, image, 1, 1))
    cross, square = wide[:, Q : 2 * Q], wide[:, 2 * Q :]
    both = jnp.where(lower((Q, Q)), gram, square)
    sums[:Q] = jnp.concatenate([cross, both], axis=1)
    along = jnp.sum(jnp.where(diagonal((Q, Q)), gram, 0.0), axis=0, keepdims=True)
    sums[Q:] = jnp.broadcast_to(jnp.concatenate([along, along], axis=1), (8, 128))


def eliminate(matrix):
    slabs = [matrix[8 * r : 8 * r + 8] for r in range(8)]
    sub = lax.broadcasted_iota(jnp.int32, (8, 128), 0)
    for k in range(8):
        spread = [
            [jnp.broadcast_to(slabs[r][:, 8 * k + j : 8 * k + j + 1], (8, 128)) for j in range(8)]
            for r in range(8)
        ]
        own, pivot = spread[k], slabs[k]
        for j in range(8):
            inverse = 1.0 / jnp.broadcast_to(own[j][j : j + 1], (8, 128))
            at = sub == j

            def cleared(value):
                row = jnp.broadcast_to(value[j : j + 1], (8, 128)) * inverse
                return jnp.where(at, row, value - own[j] * row)

            pivot = cleared(pivot)
            own = own[: j + 1] + [cleared(c) for c in own[j + 1 :]]
        for r in range(8):
            if r != k:
                for j in range(8):
                    slabs[r] = slabs[r] - spread[r][j] * jnp.broadcast_to(
                        pivot[j : j + 1], (8, 128)
                    )
        slabs[k] = pivot
    return jnp.concatenate(slabs, axis=0)[:, Q:]


def invert(gram, out):
    out[...] = eliminate(jnp.concatenate([gram[...], diagonal((Q, Q)).astype(jnp.float32)], axis=1))


def pair_sum(a, b, inverse, out, inverse_out):
    inverse_out[...] = inverse[...]
    total = a[...] + b[...]
    for j in range(G):
        out[j] = total


def chip_sum(pieces, out):
    total = summed(pieces)
    for j in range(G):
        out[j] = total


def finish(pieces, gram, inverse, image, kept, x_out, r_out, d_out):
    total = summed(pieces)
    cross, both = total[:Q, :Q], total[:Q, Q:]
    below, at = lower((Q, Q)), diagonal((Q, Q))
    under = jnp.where(below, both, 0.0)
    over = both - under
    matrix = jnp.where(at, total[Q : Q + 1, :Q], under + under.T)
    square = over + jnp.where(below, over.T, 0.0)
    res = gram[...]
    direction = kept[DIR : DIR + Q]
    step = eliminate(jnp.concatenate([matrix, res], axis=1))
    x_out[...] = kept[ITER : ITER + Q] + dot(step, direction, 0, 0)
    new_res = kept[RES : RES + Q] - dot(step, image[...], 0, 0)
    r_out[...] = new_res
    new_gram = res - dot(cross, step, 0, 0) + dot(step, dot(square, step) - cross, 0, 0)
    d_out[...] = new_res + dot(dot(inverse[...], new_gram), direction, 0, 0)


def swapped(value):
    return lax.ppermute(value, "core", [(0, 1), (1, 0)])


def across(value, k):
    return lax.ppermute(value, "z", [(i, i ^ k) for i in range(4)])


def exchanged(value, axes):
    return lax.all_to_all(value, axes, 0, 0, tiled=True)


def on_device(points, lengthscales, noise_level, iterate, residual, direction):
    rows, own, kept = call(
        prep,
        [f32(R, N, F), f32(ROWS, 128), f32(NOISE + 8, 128)],
        [
            [pltpu.VMEM((N, F), jnp.float32), pltpu.VMEM((1, F), jnp.float32)],
            pltpu.SemaphoreType.DMA((5,)),
        ],
        room=ROOM,
        ins=[HBM, HBM, pl.BlockSpec(memory_space=pltpu.SMEM), HBM, HBM, HBM],
    )(
        points,
        lengthscales.reshape(1, F),
        noise_level,
        iterate.T,
        residual.T,
        direction.T,
    )
    rows = exchanged(rows, PLANE)
    mine = [own] + [across(own, k) for k in range(1, 4)]
    cols = mine + [swapped(m) for m in mine]
    spread = call(
        spread_cols,
        [
            jax.ShapeDtypeStruct((C * N, 6 * F), jnp.bfloat16),
            jax.ShapeDtypeStruct((2 * Q, C * N), jnp.bfloat16),
            f32(8, C * N),
            f32(Q // 2, 128),
        ],
        flops=10**8,
    )(*cols)
    sent = call(
        products,
        f32(R, Q + Q // 2, 128),
        [pltpu.VMEM((TILE, 6 * F), jnp.bfloat16)],
        8 * 10**9,
        24,
    )(rows, *spread)
    image, gram, sums = call(grams, [f32(Q, N), f32(Q, Q), f32(SUMS, 128)])(
        exchanged(sent, PLANE), kept
    )
    inverse = call(invert, f32(Q, Q), flops=10**8)(gram)
    both, inverse = call(pair_sum, [f32(G, SUMS, 128), f32(Q, Q)])(sums, swapped(sums), inverse)
    by_chip = call(chip_sum, f32(G, SUMS, 128))(exchanged(both, CHIPS))
    whole = exchanged(by_chip, BLK)
    outs = call(finish, [f32(Q, N)] * 3)(whole, gram, inverse, image, kept)
    return tuple(o.T for o in outs)


def solution(mesh):
    fine = Mesh(mesh.devices.reshape(4, 2, 4, 2, 2), AXES)
    split_rows = P(AXES, None)
    return jax.shard_map(
        on_device,
        mesh=fine,
        in_specs=(split_rows, P(), P(), split_rows, split_rows, split_rows),
        out_specs=(split_rows,) * 3,
        check_vma=False,
    )
```

```python
import math

import jax
import jax.numpy as jnp
from jax import lax
from jax.experimental import pallas as pl
from jax.experimental.pallas import tpu as pltpu
from jax.sharding import Mesh, PartitionSpec as P

AXES = ("y", "xl", "z", "xh", "core")
PLANE = ("y", "xl", "xh")
N = 128
F = 128
Q = 64
R = 16
C = 8
TILE = 1024
CHUNK = 256
HI = lax.Precision.HIGHEST
ROOT = math.sqrt(math.log2(math.e))
DIRS = N + Q
GRAM = DIRS + Q // 2
ROWS = GRAM + 8
ITER, RES, DIR, NOISE = 0, Q, 2 * Q, 3 * Q
SUMS = Q + 8
HBM = pl.BlockSpec(memory_space=pltpu.MemorySpace.HBM)
ROOM = 62
VM = pl.BlockSpec(memory_space=pltpu.VMEM)


def call(body, outs, scratch=(), flops=10**6, room=4, ins=None):
    return pl.pallas_call(
        body,
        out_shape=outs,
        **({} if ins is None else {"in_specs": ins}),
        out_specs=jax.tree.map(lambda _: VM, outs),
        scratch_shapes=list(scratch),
        compiler_params=pltpu.CompilerParams(vmem_limit_bytes=room * 2**20),
        cost_estimate=pl.CostEstimate(flops=flops, bytes_accessed=10**6, transcendentals=0),
    )


def f32(*shape):
    return jax.ShapeDtypeStruct(shape, jnp.float32)


def dot(a, b, ca=1, cb=0, precision=HI):
    return lax.dot_general(
        a, b, (((ca,), (cb,)), ((), ())), precision=precision, preferred_element_type=jnp.float32
    )


def low_lanes(shape):
    return lax.broadcasted_iota(jnp.int32, shape, 1) < Q


def fold(wide):
    half = wide.shape[0] // 2
    return jnp.where(low_lanes((half, 128)), wide[:half], wide[half:])


def unfold(packed):
    return jnp.concatenate([packed[:, :Q], packed[:, Q:]], axis=0)


def prep(points, scales, noise, iterate, residual, direction, rows, cols, kept, place, sems):
    points_in, scales_in = place
    copies = [
        pltpu.make_async_copy(points, points_in, sems.at[0]),
        pltpu.make_async_copy(scales, scales_in, sems.at[1]),
        pltpu.make_async_copy(residual, kept.at[RES : RES + Q], sems.at[2]),
        pltpu.make_async_copy(direction, kept.at[DIR : DIR + Q], sems.at[3]),
        pltpu.make_async_copy(iterate, kept.at[ITER : ITER + Q], sems.at[4]),
    ]
    for copy in copies:
        copy.start()
    for copy in copies[:2]:
        copy.wait()
    unit = points_in[...] / scales_in[...] * ROOT
    half = 0.5 * jnp.sum(unit * unit, axis=1, keepdims=True)
    for i in range(R):
        rows[i] = unit
    cols[:N] = unit
    for copy in copies[2:]:
        copy.wait()
    residual = kept[RES : RES + Q]
    cols[N:DIRS] = kept[DIR : DIR + Q]
    cols[DIRS:GRAM] = fold(dot(residual, jnp.concatenate([residual, residual], axis=0), 1, 1))
    cols[GRAM:] = jnp.broadcast_to(half, (N, N)).T[:8]
    kept[NOISE:] = jnp.full((8, 128), noise[0])


def split(value):
    top = value.astype(jnp.bfloat16)
    rest = value - top.astype(jnp.float32)
    mid = rest.astype(jnp.bfloat16)
    low = (rest - mid.astype(jnp.float32)).astype(jnp.bfloat16)
    return top, mid, low


def spread_cols(*refs):
    cols, (right, dirs, halves, gram) = refs[:C], refs[C:]
    total = cols[0][DIRS:GRAM]
    for j in range(C):
        at = slice(j * N, (j + 1) * N)
        top, mid, low = split(cols[j][:N])
        right[at] = jnp.concatenate([top, mid, top, low, top, mid], axis=1)
        high, rest, _ = split(cols[j][N:DIRS])
        dirs[:, at] = jnp.concatenate([high, rest], axis=0)
        halves[:, at] = cols[j][GRAM:]
        if j > 0:
            total += cols[j][DIRS:GRAM]
    gram[...] = total


def products(rows, right, dirs, halves, gram, out, left):
    per = TILE // N

    def step(i, carry):
        unit = rows[pl.ds(i * per, per)].reshape(TILE, F)
        top, mid, low = split(unit)
        left[...] = jnp.concatenate([top, top, mid, top, low, mid], axis=1)
        half = 0.5 * jnp.sum(unit * unit, axis=1, keepdims=True)
        total = jnp.zeros((TILE, 2 * Q), jnp.float32)
        for j in range(C * N // CHUNK):
            at = slice(j * CHUNK, (j + 1) * CHUNK)
            inner = dot(left[...], right[at], 1, 1, None)
            kernel = jnp.exp2(inner - half - halves[0:1, at])
            high = kernel.astype(jnp.bfloat16)
            rest = (kernel - high.astype(jnp.float32)).astype(jnp.bfloat16)
            weights = jnp.concatenate([dirs[:, at], dirs[:, at]], axis=1)
            total += dot(jnp.concatenate([high, rest], axis=1), weights, 1, 1, None)
        total += pltpu.roll(total, Q, 1)
        for b in range(per):
            out[i * per + b, :Q] = fold(total[b * N : (b + 1) * N])
            out[i * per + b, Q:] = gram[...]
        return carry

    lax.fori_loop(0, R // per, step, 0)


def summed(pieces):
    total = pieces[0]
    for j in range(1, pieces.shape[0]):
        total += pieces[j]
    return total


def lower(shape):
    return lax.broadcasted_iota(jnp.int32, shape, 0) > lax.broadcasted_iota(jnp.int32, shape, 1)


def diagonal(shape):
    return lax.broadcasted_iota(jnp.int32, shape, 0) == lax.broadcasted_iota(jnp.int32, shape, 1)


def grams(pieces, kept, image_out, gram_out, sums):
    total = summed(pieces)
    turned = total[:Q].T
    direction = kept[DIR : DIR + Q]
    image = jnp.concatenate([turned[:Q], turned[Q:]], axis=1) + kept[NOISE : NOISE + 1] * direction
    image_out[...] = image
    gram_out[...] = unfold(total[Q:])
    side = jnp.concatenate([direction, kept[RES : RES + Q], image], axis=0)
    wide = dot(image, side, 1, 1)
    gram = 0.5 * (wide[:, :Q] + dot(direction, image, 1, 1))
    cross, square = wide[:, Q : 2 * Q], wide[:, 2 * Q :]
    both = jnp.where(lower((Q, Q)), gram, square)
    sums[:Q] = jnp.concatenate([cross, both], axis=1)
    along = jnp.sum(jnp.where(diagonal((Q, Q)), gram, 0.0), axis=0, keepdims=True)
    sums[Q:] = jnp.broadcast_to(jnp.concatenate([along, along], axis=1), (8, 128))


def eliminate(matrix):
    slabs = [matrix[8 * r : 8 * r + 8] for r in range(8)]
    sub = lax.broadcasted_iota(jnp.int32, (8, 128), 0)
    for k in range(8):
        spread = [
            [jnp.broadcast_to(slabs[r][:, 8 * k + j : 8 * k + j + 1], (8, 128)) for j in range(8)]
            for r in range(8)
        ]
        own, pivot = spread[k], slabs[k]
        for j in range(8):
            inverse = 1.0 / jnp.broadcast_to(own[j][j : j + 1], (8, 128))
            at = sub == j

            def cleared(value):
                row = jnp.broadcast_to(value[j : j + 1], (8, 128)) * inverse
                return jnp.where(at, row, value - own[j] * row)

            pivot = cleared(pivot)
            own = own[: j + 1] + [cleared(c) for c in own[j + 1 :]]
        for r in range(8):
            if r != k:
                for j in range(8):
                    slabs[r] = slabs[r] - spread[r][j] * jnp.broadcast_to(
                        pivot[j : j + 1], (8, 128)
                    )
        slabs[k] = pivot
    return jnp.concatenate(slabs, axis=0)[:, Q:]


def invert(gram, out):
    out[...] = eliminate(jnp.concatenate([gram[...], diagonal((Q, Q)).astype(jnp.float32)], axis=1))


def z_sum(a, b, c, d, inverse, out, inverse_out):
    inverse_out[...] = inverse[...]
    out[...] = (a[...] + b[...]) + (c[...] + d[...])


def pair_sum(a, b, out):
    total = a[...] + b[...]
    for j in range(R):
        out[j] = total


def finish(pieces, gram, inverse, image, kept, x_out, r_out, d_out):
    total = summed(pieces)
    cross, both = total[:Q, :Q], total[:Q, Q:]
    below, at = lower((Q, Q)), diagonal((Q, Q))
    under = jnp.where(below, both, 0.0)
    over = both - under
    matrix = jnp.where(at, total[Q : Q + 1, :Q], under + under.T)
    square = over + jnp.where(below, over.T, 0.0)
    res = gram[...]
    direction = kept[DIR : DIR + Q]
    step = eliminate(jnp.concatenate([matrix, res], axis=1))
    x_out[...] = kept[ITER : ITER + Q] + dot(step, direction, 0, 0)
    new_res = kept[RES : RES + Q] - dot(step, image[...], 0, 0)
    r_out[...] = new_res
    new_gram = res - dot(cross, step, 0, 0) + dot(step, dot(square, step) - cross, 0, 0)
    d_out[...] = new_res + dot(dot(inverse[...], new_gram), direction, 0, 0)


def swapped(value):
    return lax.ppermute(value, "core", [(0, 1), (1, 0)])


def across(value, k):
    return lax.ppermute(value, "z", [(i, i ^ k) for i in range(4)])


def exchanged(value, axes):
    return lax.all_to_all(value, axes, 0, 0, tiled=True)


def on_device(points, lengthscales, noise_level, iterate, residual, direction):
    rows, own, kept = call(
        prep,
        [f32(R, N, F), f32(ROWS, 128), f32(NOISE + 8, 128)],
        [
            [pltpu.VMEM((N, F), jnp.float32), pltpu.VMEM((1, F), jnp.float32)],
            pltpu.SemaphoreType.DMA((5,)),
        ],
        room=ROOM,
        ins=[HBM, HBM, pl.BlockSpec(memory_space=pltpu.SMEM), HBM, HBM, HBM],
    )(
        points,
        lengthscales.reshape(1, F),
        noise_level,
        iterate.T,
        residual.T,
        direction.T,
    )
    rows = exchanged(rows, PLANE)
    mine = [own] + [across(own, k) for k in range(1, 4)]
    cols = mine + [swapped(m) for m in mine]
    spread = call(
        spread_cols,
        [
            jax.ShapeDtypeStruct((C * N, 6 * F), jnp.bfloat16),
            jax.ShapeDtypeStruct((2 * Q, C * N), jnp.bfloat16),
            f32(8, C * N),
            f32(Q // 2, 128),
        ],
        flops=10**8,
    )(*cols)
    sent = call(
        products,
        f32(R, Q + Q // 2, 128),
        [pltpu.VMEM((TILE, 6 * F), jnp.bfloat16)],
        8 * 10**9,
        24,
    )(rows, *spread)
    image, gram, sums = call(grams, [f32(Q, N), f32(Q, Q), f32(SUMS, 128)])(
        exchanged(sent, PLANE), kept
    )
    inverse = call(invert, f32(Q, Q), flops=10**8)(gram)
    column, inverse = call(z_sum, [f32(SUMS, 128), f32(Q, Q)])(
        sums, *[across(sums, k) for k in range(1, 4)], inverse
    )
    both = call(pair_sum, f32(R, SUMS, 128))(column, swapped(column))
    whole = exchanged(both, PLANE)
    outs = call(finish, [f32(Q, N)] * 3)(whole, gram, inverse, image, kept)
    return tuple(o.T for o in outs)


def solution(mesh):
    fine = Mesh(mesh.devices.reshape(4, 2, 4, 2, 2), AXES)
    split_rows = P(AXES, None)
    return jax.shard_map(
        on_device,
        mesh=fine,
        in_specs=(split_rows, P(), P(), split_rows, split_rows, split_rows),
        out_specs=(split_rows,) * 3,
        check_vma=False,
    )
```

```python
import math

import jax
import jax.numpy as jnp
from jax import lax
from jax.experimental import pallas as pl
from jax.experimental.pallas import tpu as pltpu
from jax.sharding import Mesh, PartitionSpec as P

AXES = ("y", "xl", "z", "xh", "core")
PLANE = ("y", "xl", "xh")
N = 128
F = 128
Q = 64
R = 16
Z = 4
CHUNK = 256
H = Q // 2
HI = lax.Precision.HIGHEST
ROOT = math.sqrt(math.log2(math.e))
DIRS = N + Q
COLS = DIRS + 8
ROWS = DIRS + Q
ITER, RES, DIR = 0, Q, 2 * Q
DIAG, GRAM, SUMS = Q, Q + 8, Q + 32
SMEM = pl.BlockSpec(memory_space=pltpu.SMEM)
HBM = pl.BlockSpec(memory_space=pltpu.MemorySpace.HBM)
ROOM = 62
VM = pl.BlockSpec(memory_space=pltpu.VMEM)


def call(body, outs, scratch=(), flops=10**6, room=4, ins=None):
    return pl.pallas_call(
        body,
        out_shape=outs,
        **({} if ins is None else {"in_specs": ins}),
        out_specs=jax.tree.map(lambda _: VM, outs),
        scratch_shapes=list(scratch),
        compiler_params=pltpu.CompilerParams(vmem_limit_bytes=room * 2**20),
        cost_estimate=pl.CostEstimate(flops=flops, bytes_accessed=10**6, transcendentals=0),
    )


def f32(*shape):
    return jax.ShapeDtypeStruct(shape, jnp.float32)


def dot(a, b, ca=1, cb=0, precision=HI):
    return lax.dot_general(
        a, b, (((ca,), (cb,)), ((), ())), precision=precision, preferred_element_type=jnp.float32
    )


def low_lanes(shape):
    return lax.broadcasted_iota(jnp.int32, shape, 1) < Q


def fold(wide):
    half = wide.shape[0] // 2
    return jnp.where(low_lanes((half, 128)), wide[:half], wide[half:])


def unfold(packed):
    return jnp.concatenate([packed[:, :Q], packed[:, Q:]], axis=0)


def prep(points, scales, iterate, residual, direction, rows, cols, kept, place, sems):
    points_in, scales_in = place
    copies = [
        pltpu.make_async_copy(points, points_in, sems.at[0]),
        pltpu.make_async_copy(scales, scales_in, sems.at[1]),
        pltpu.make_async_copy(residual, kept.at[RES : RES + Q], sems.at[2]),
        pltpu.make_async_copy(direction, kept.at[DIR : DIR + Q], sems.at[3]),
        pltpu.make_async_copy(iterate, kept.at[ITER : ITER + Q], sems.at[4]),
    ]
    for copy in copies:
        copy.start()
    for copy in copies[:2]:
        copy.wait()
    unit = points_in[...] / scales_in[...] * ROOT
    half = 0.5 * jnp.sum(unit * unit, axis=1, keepdims=True)
    as_row = jnp.broadcast_to(half, (N, N)).T[:8]
    for copy in copies[2:]:
        copy.wait()
    for i in range(R):
        cols[i, :N] = unit
        cols[i, N:DIRS] = kept[DIR : DIR + Q]
        cols[i, DIRS:] = as_row
    rows[:N] = unit
    rows[N:DIRS] = kept[DIR : DIR + Q]
    rows[DIRS:] = kept[RES : RES + Q]


def split(value):
    top = value.astype(jnp.bfloat16)
    rest = value - top.astype(jnp.float32)
    mid = rest.astype(jnp.bfloat16)
    low = (rest - mid.astype(jnp.float32)).astype(jnp.bfloat16)
    return top, mid, low


def halved(residual):
    wide = dot(residual, jnp.concatenate([residual, residual], axis=0), 1, 1)
    corner = dot(residual[H:], jnp.concatenate([residual[H:]] * 4, axis=0), 1, 1)
    group = lax.broadcasted_iota(jnp.int32, (8, 128), 1) // H
    last = corner[:8]
    for g in range(1, 4):
        last = jnp.where(group == g, corner[8 * g : 8 * g + 8], last)
    return jnp.concatenate([fold(wide[:H]), last], axis=0)


def restored(packed):
    top = unfold(packed[:16])
    corner = jnp.concatenate([packed[16:, H * g : H * (g + 1)] for g in range(4)], axis=0)
    under = jnp.concatenate([jnp.zeros((H, H), jnp.float32), corner], axis=1)
    full = jnp.concatenate([top, under], axis=0)
    row = lax.broadcasted_iota(jnp.int32, (Q, Q), 0)
    column = lax.broadcasted_iota(jnp.int32, (Q, Q), 1)
    return jnp.where((row >= H) & (column < H), full.T, full)


def spread_rows(a, b, c, d, left, halves, side, gram):
    for k, rows in enumerate((a, b, c, d)):
        at = slice(k * N, (k + 1) * N)
        unit = rows[:N]
        top, mid, low = split(unit)
        left[at] = jnp.concatenate([top, top, mid, top, low, mid], axis=1)
        half = 0.5 * jnp.sum(unit * unit, axis=1, keepdims=True)
        halves[at] = jnp.broadcast_to(half, (N, CHUNK))
        side[:, at] = rows[N:]
    residual = side[Q:]
    gram[...] = halved(residual)


def partial(left, own, cols, right, dirs, halves):
    for j in range(R):
        at = slice(j * N, (j + 1) * N)
        top, mid, low = split(cols[j, :N])
        right[at] = jnp.concatenate([top, mid, top, low, top, mid], axis=1)
        high, rest, _ = split(cols[j, N:DIRS])
        dirs[:, at] = jnp.concatenate([high, rest], axis=0)
        halves[:, at] = cols[j, DIRS:]
    total = jnp.zeros((Z * N, 2 * Q), jnp.float32)
    for j in range(R * N // CHUNK):
        at = slice(j * CHUNK, (j + 1) * CHUNK)
        inner = dot(left[...], right[at], 1, 1, None)
        kernel = jnp.exp2(inner - own[...] - halves[0:1, at])
        high = kernel.astype(jnp.bfloat16)
        rest = (kernel - high.astype(jnp.float32)).astype(jnp.bfloat16)
        weights = jnp.concatenate([dirs[:, at], dirs[:, at]], axis=1)
        total += dot(jnp.concatenate([high, rest], axis=1), weights, 1, 1, None)
    return total


def products_first(left, own, cols, out, right, dirs, halves):
    out[...] = partial(left, own, cols, right, dirs, halves)


def products_last(left, own, cols, before, out, right, dirs, halves):
    total = before[...] + partial(left, own, cols, right, dirs, halves)
    total += pltpu.roll(total, Q, 1)
    for k in range(Z):
        out[k * Q : (k + 1) * Q] = fold(total[k * N : (k + 1) * N])


def summed(pieces):
    total = pieces[0]
    for j in range(1, pieces.shape[0]):
        total += pieces[j]
    return total


def lower(shape):
    return lax.broadcasted_iota(jnp.int32, shape, 0) > lax.broadcasted_iota(jnp.int32, shape, 1)


def diagonal(shape):
    return lax.broadcasted_iota(jnp.int32, shape, 0) == lax.broadcasted_iota(jnp.int32, shape, 1)


def grams(a, b, c, d, sides, res_gram, noise, image_out, sums):
    pieces = (a, b, c, d)
    parts = []
    for k in range(Z):
        total = a[k * Q : (k + 1) * Q]
        for place in range(1, Z):
            total += pieces[place][(k ^ place) * Q : ((k ^ place) + 1) * Q]
        turned = total.T
        parts += [turned[:Q], turned[Q:]]
    direction = sides[:Q]
    image = jnp.concatenate(parts, axis=1) + noise[0, 0] * direction
    image_out[...] = image[:, :N]
    wide = dot(image, jnp.concatenate([sides[...], image], axis=0), 1, 1)
    gram = 0.5 * (wide[:, :Q] + dot(direction, image, 1, 1))
    cross, square = wide[:, Q : 2 * Q], wide[:, 2 * Q :]
    both = jnp.where(lower((Q, Q)), gram, square)
    sums[:Q] = jnp.concatenate([cross, both], axis=1)
    along = jnp.sum(jnp.where(diagonal((Q, Q)), gram, 0.0), axis=0, keepdims=True)
    sums[DIAG:GRAM] = jnp.broadcast_to(jnp.concatenate([along, along], axis=1), (8, 128))
    sums[GRAM:] = res_gram[...]


def eliminate(*matrices):
    sub = lax.broadcasted_iota(jnp.int32, (8, 128), 0)
    each = range(len(matrices))
    slabs = [[m[8 * r : 8 * r + 8] for r in range(8)] for m in matrices]
    for k in range(8):
        spread = [
            [
                [
                    jnp.broadcast_to(slabs[m][r][:, 8 * k + j : 8 * k + j + 1], (8, 128))
                    for j in range(8)
                ]
                for r in range(8)
            ]
            for m in each
        ]
        own = [spread[m][k] for m in each]
        pivot = [slabs[m][k] for m in each]
        for j in range(8):
            inverse = [1.0 / jnp.broadcast_to(own[m][j][j : j + 1], (8, 128)) for m in each]

            def cleared(value, m):
                row = jnp.broadcast_to(value[j : j + 1], (8, 128)) * inverse[m]
                return jnp.where(sub == j, row, value - own[m][j] * row)

            pivot = [cleared(pivot[m], m) for m in each]
            own = [own[m][: j + 1] + [cleared(c, m) for c in own[m][j + 1 :]] for m in each]
        for r in range(8):
            if r != k:
                for j in range(8):
                    for m in each:
                        slabs[m][r] = slabs[m][r] - spread[m][r][j] * jnp.broadcast_to(
                            pivot[m][j : j + 1], (8, 128)
                        )
        for m in each:
            slabs[m][k] = pivot[m]
    return [jnp.concatenate(rows, axis=0)[:, Q:] for rows in slabs]


def half_of(core, total):
    return jnp.where(core[0] == 0, total[: SUMS // 2], total[SUMS // 2 :])


def pair_sum(core, a, b, out):
    total = half_of(core, a[...] + b[...])
    for j in range(R):
        out[j] = total


def plane_sum(pieces, out):
    out[...] = summed(pieces)


def finish(core, mine, theirs, image, kept, x_out, r_out, d_out):
    first = core[0] == 0
    mine, theirs = mine[...], theirs[...]
    total = jnp.concatenate(
        [jnp.where(first, mine, theirs), jnp.where(first, theirs, mine)], axis=0
    )
    cross, both = total[:Q, :Q], total[:Q, Q:]
    below, at = lower((Q, Q)), diagonal((Q, Q))
    under = jnp.where(below, both, 0.0)
    over = both - under
    matrix = jnp.where(at, total[DIAG : DIAG + 1, :Q], under + under.T)
    square = over + jnp.where(below, over.T, 0.0)
    res = restored(total[GRAM:])
    direction = kept[DIR : DIR + Q]
    step, inverse = eliminate(
        jnp.concatenate([matrix, res], axis=1),
        jnp.concatenate([res, at.astype(jnp.float32)], axis=1),
    )
    x_out[...] = kept[ITER : ITER + Q] + dot(step, direction, 0, 0)
    new_res = kept[RES : RES + Q] - dot(step, image[...], 0, 0)
    r_out[...] = new_res
    new_gram = res - dot(cross, step, 0, 0) + dot(step, dot(square, step) - cross, 0, 0)
    d_out[...] = new_res + dot(dot(inverse, new_gram), direction, 0, 0)


def swapped(value):
    return lax.ppermute(value, "core", [(0, 1), (1, 0)])


def across(value, k):
    return lax.ppermute(value, "z", [(i, i ^ k) for i in range(4)])


def exchanged(value, axes):
    return lax.all_to_all(value, axes, 0, 0, tiled=True)


def on_device(points, lengthscales, noise_level, iterate, residual, direction):
    own, cols, kept = call(
        prep,
        [f32(ROWS, 128), f32(R, COLS, 128), f32(3 * Q, 128)],
        [
            [pltpu.VMEM((N, F), jnp.float32), pltpu.VMEM((1, F), jnp.float32)],
            pltpu.SemaphoreType.DMA((5,)),
        ],
        room=ROOM,
        ins=[HBM] * 5,
    )(
        points,
        lengthscales.reshape(1, F),
        iterate.T,
        residual.T,
        direction.T,
    )
    cols = exchanged(cols, PLANE)
    rows = [own] + [across(own, k) for k in range(1, Z)]
    left, halves, sides, res_gram = call(
        spread_rows,
        [
            jax.ShapeDtypeStruct((Z * N, 6 * F), jnp.bfloat16),
            f32(Z * N, CHUNK),
            f32(2 * Q, Z * N),
            f32(SUMS - GRAM, 128),
        ],
        flops=10**8,
    )(*rows)
    other = swapped(cols)
    scratch = [
        pltpu.VMEM((R * N, 6 * F), jnp.bfloat16),
        pltpu.VMEM((2 * Q, R * N), jnp.bfloat16),
        pltpu.VMEM((8, R * N), jnp.float32),
    ]
    part = call(products_first, f32(Z * N, 2 * Q), scratch, 4 * 10**9, 24)(left, halves, cols)
    sent = call(products_last, f32(Z * Q, 128), scratch, 4 * 10**9, 24)(
        left, halves, other, part
    )
    got = [sent] + [across(sent, k) for k in range(1, Z)]
    image, sums = call(grams, [f32(Q, N), f32(SUMS, 128)])(
        *got, sides, res_gram, noise_level.reshape(1, 1)
    )
    core = lax.axis_index("core").reshape(1)
    both = call(pair_sum, f32(R, SUMS // 2, 128), ins=[SMEM, VM, VM])(core, sums, swapped(sums))
    half = call(plane_sum, f32(SUMS // 2, 128))(exchanged(both, PLANE))
    outs = call(finish, [f32(Q, N)] * 3, ins=[SMEM] + [VM] * 4)(
        core, half, swapped(half), image, kept
    )
    return tuple(o.T for o in outs)


def solution(mesh):
    fine = Mesh(mesh.devices.reshape(4, 2, 4, 2, 2), AXES)
    split_rows = P(AXES, None)
    return jax.shard_map(
        on_device,
        mesh=fine,
        in_specs=(split_rows, P(), P(), split_rows, split_rows, split_rows),
        out_specs=(split_rows,) * 3,
        check_vma=False,
    )
```

```python
import math

import jax
import jax.numpy as jnp
from jax import lax
from jax.experimental import pallas as pl
from jax.experimental.pallas import tpu as pltpu
from jax.sharding import Mesh, PartitionSpec as P

AXES = ("y", "xl", "z", "xh", "core")
PLANE = ("y", "xl", "xh")
N = 128
F = 128
Q = 64
R = 16
Z = 4
CHUNK = 256
H = Q // 2
HI = lax.Precision.HIGHEST
ROOT = math.sqrt(math.log2(math.e))
DIRS = N + Q
COLS = DIRS + 8
ROWS = DIRS + Q
ITER, RES, DIR = 0, Q, 2 * Q
DIAG, GRAM, SUMS = Q, Q + 8, Q + 32
SMEM = pl.BlockSpec(memory_space=pltpu.SMEM)
HBM = pl.BlockSpec(memory_space=pltpu.MemorySpace.HBM)
ROOM = 62
VM = pl.BlockSpec(memory_space=pltpu.VMEM)


def call(body, outs, scratch=(), flops=10**6, room=4, ins=None):
    return pl.pallas_call(
        body,
        out_shape=outs,
        **({} if ins is None else {"in_specs": ins}),
        out_specs=jax.tree.map(lambda _: VM, outs),
        scratch_shapes=list(scratch),
        compiler_params=pltpu.CompilerParams(vmem_limit_bytes=room * 2**20),
        cost_estimate=pl.CostEstimate(flops=flops, bytes_accessed=10**6, transcendentals=0),
    )


def f32(*shape):
    return jax.ShapeDtypeStruct(shape, jnp.float32)


def dot(a, b, ca=1, cb=0, precision=HI):
    return lax.dot_general(
        a, b, (((ca,), (cb,)), ((), ())), precision=precision, preferred_element_type=jnp.float32
    )


def low_lanes(shape):
    return lax.broadcasted_iota(jnp.int32, shape, 1) < Q


def fold(wide):
    half = wide.shape[0] // 2
    return jnp.where(low_lanes((half, 128)), wide[:half], wide[half:])


def unfold(packed):
    return jnp.concatenate([packed[:, :Q], packed[:, Q:]], axis=0)


def prep(points, scales, iterate, residual, direction, rows, cols, kept, place, sems):
    points_in, scales_in = place
    copies = [
        pltpu.make_async_copy(points, points_in, sems.at[0]),
        pltpu.make_async_copy(scales, scales_in, sems.at[1]),
        pltpu.make_async_copy(residual, kept.at[RES : RES + Q], sems.at[2]),
        pltpu.make_async_copy(direction, kept.at[DIR : DIR + Q], sems.at[3]),
        pltpu.make_async_copy(iterate, kept.at[ITER : ITER + Q], sems.at[4]),
    ]
    for copy in copies:
        copy.start()
    for copy in copies[:2]:
        copy.wait()
    unit = points_in[...] / scales_in[...] * ROOT
    half = 0.5 * jnp.sum(unit * unit, axis=1, keepdims=True)
    as_row = jnp.broadcast_to(half, (N, N)).T[:8]
    for copy in copies[2:]:
        copy.wait()
    for i in range(R):
        cols[i, :N] = unit
        cols[i, N:DIRS] = kept[DIR : DIR + Q]
        cols[i, DIRS:] = as_row
    rows[:N] = unit
    rows[N:DIRS] = kept[DIR : DIR + Q]
    rows[DIRS:] = kept[RES : RES + Q]


def split(value):
    top = value.astype(jnp.bfloat16)
    rest = value - top.astype(jnp.float32)
    mid = rest.astype(jnp.bfloat16)
    low = (rest - mid.astype(jnp.float32)).astype(jnp.bfloat16)
    return top, mid, low


def halved(residual):
    wide = dot(residual, jnp.concatenate([residual, residual], axis=0), 1, 1)
    corner = dot(residual[H:], jnp.concatenate([residual[H:]] * 4, axis=0), 1, 1)
    group = lax.broadcasted_iota(jnp.int32, (8, 128), 1) // H
    last = corner[:8]
    for g in range(1, 4):
        last = jnp.where(group == g, corner[8 * g : 8 * g + 8], last)
    return jnp.concatenate([fold(wide[:H]), last], axis=0)


def restored(packed):
    top = unfold(packed[:16])
    corner = jnp.concatenate([packed[16:, H * g : H * (g + 1)] for g in range(4)], axis=0)
    under = jnp.concatenate([jnp.zeros((H, H), jnp.float32), corner], axis=1)
    full = jnp.concatenate([top, under], axis=0)
    row = lax.broadcasted_iota(jnp.int32, (Q, Q), 0)
    column = lax.broadcasted_iota(jnp.int32, (Q, Q), 1)
    return jnp.where((row >= H) & (column < H), full.T, full)


def spread_rows(a, b, c, d, left, halves, side, gram):
    for k, rows in enumerate((a, b, c, d)):
        at = slice(k * N, (k + 1) * N)
        unit = rows[:N]
        top, mid, low = split(unit)
        left[at] = jnp.concatenate([top, top, mid, top, low, mid], axis=1)
        half = 0.5 * jnp.sum(unit * unit, axis=1, keepdims=True)
        halves[at] = jnp.broadcast_to(half, (N, CHUNK))
        side[:, at] = rows[N:]
    residual = side[Q:]
    gram[...] = halved(residual)


def partial(left, own, cols, total):
    per = CHUNK // N
    for j in range(R // per):
        blocks = [cols[j * per + i] for i in range(per)]
        tops = [split(b[:N]) for b in blocks]
        right = jnp.concatenate(
            [jnp.concatenate([t, m, t, w, t, m], axis=1) for t, m, w in tops], axis=0
        )
        pairs = [split(b[N:DIRS]) for b in blocks]
        dirs = jnp.concatenate([jnp.concatenate(p[:2], axis=0) for p in pairs], axis=1)
        half = jnp.concatenate([b[DIRS : DIRS + 1] for b in blocks], axis=1)
        inner = dot(left[...], right, 1, 1, None)
        kernel = jnp.exp2(inner - own[...] - half)
        high = kernel.astype(jnp.bfloat16)
        rest = (kernel - high.astype(jnp.float32)).astype(jnp.bfloat16)
        weights = jnp.concatenate([dirs, dirs], axis=1)
        total += dot(jnp.concatenate([high, rest], axis=1), weights, 1, 1, None)
    return total


def products_first(left, own, cols, out):
    out[...] = partial(left, own, cols, jnp.zeros((Z * N, 2 * Q), jnp.float32))


def products_last(left, own, cols, before, up, down):
    total = partial(left, own, cols, before[...])
    total += pltpu.roll(total, Q, 1)
    for k in range(Z):
        block = fold(total[k * N : (k + 1) * N])
        up[k * H : (k + 1) * H] = block[:H]
        down[k * H : (k + 1) * H] = block[H:]


def met(mine, theirs, place):
    return [
        mine[k * H : (k + 1) * H] + theirs[(k ^ place) * H : ((k ^ place) + 1) * H]
        for k in range(Z)
    ]


def half_way(up, up_theirs, down, down_theirs, up_out, down_out):
    up_out[...] = jnp.concatenate(met(up, up_theirs, 1), axis=0)
    down_out[...] = jnp.concatenate(met(down, down_theirs, 3), axis=0)


def summed(pieces):
    total = pieces[0]
    for j in range(1, pieces.shape[0]):
        total += pieces[j]
    return total


def lower(shape):
    return lax.broadcasted_iota(jnp.int32, shape, 0) > lax.broadcasted_iota(jnp.int32, shape, 1)


def diagonal(shape):
    return lax.broadcasted_iota(jnp.int32, shape, 0) == lax.broadcasted_iota(jnp.int32, shape, 1)


def grams(up, up_theirs, down, down_theirs, sides, res_gram, noise, image_out, sums):
    parts = []
    for block in zip(met(up, up_theirs, 3), met(down, down_theirs, 1)):
        turned = jnp.concatenate(block, axis=0).T
        parts += [turned[:Q], turned[Q:]]
    direction = sides[:Q]
    image = jnp.concatenate(parts, axis=1) + noise[0, 0] * direction
    image_out[...] = image[:, :N]
    wide = dot(image, jnp.concatenate([sides[...], image], axis=0), 1, 1)
    gram = 0.5 * (wide[:, :Q] + dot(direction, image, 1, 1))
    cross, square = wide[:, Q : 2 * Q], wide[:, 2 * Q :]
    both = jnp.where(lower((Q, Q)), gram, square)
    sums[:Q] = jnp.concatenate([cross, both], axis=1)
    along = jnp.sum(jnp.where(diagonal((Q, Q)), gram, 0.0), axis=0, keepdims=True)
    sums[DIAG:GRAM] = jnp.broadcast_to(jnp.concatenate([along, along], axis=1), (8, 128))
    sums[GRAM:] = res_gram[...]


def eliminate(*matrices):
    sub = lax.broadcasted_iota(jnp.int32, (8, 128), 0)
    each = range(len(matrices))
    slabs = [[m[8 * r : 8 * r + 8] for r in range(8)] for m in matrices]
    for k in range(8):
        spread = [
            [
                [
                    jnp.broadcast_to(slabs[m][r][:, 8 * k + j : 8 * k + j + 1], (8, 128))
                    for j in range(8)
                ]
                for r in range(8)
            ]
            for m in each
        ]
        own = [spread[m][k] for m in each]
        pivot = [slabs[m][k] for m in each]
        for j in range(8):
            inverse = [1.0 / jnp.broadcast_to(own[m][j][j : j + 1], (8, 128)) for m in each]

            def cleared(value, m):
                row = jnp.broadcast_to(value[j : j + 1], (8, 128)) * inverse[m]
                return jnp.where(sub == j, row, value - own[m][j] * row)

            pivot = [cleared(pivot[m], m) for m in each]
            own = [own[m][: j + 1] + [cleared(c, m) for c in own[m][j + 1 :]] for m in each]
        for r in range(8):
            if r != k:
                for j in range(8):
                    for m in each:
                        slabs[m][r] = slabs[m][r] - spread[m][r][j] * jnp.broadcast_to(
                            pivot[m][j : j + 1], (8, 128)
                        )
        for m in each:
            slabs[m][k] = pivot[m]
    return [jnp.concatenate(rows, axis=0)[:, Q:] for rows in slabs]


def half_of(core, total):
    return jnp.where(core[0] == 0, total[: SUMS // 2], total[SUMS // 2 :])


def pair_sum(core, a, b, out):
    total = half_of(core, a[...] + b[...])
    for j in range(R):
        out[j] = total


def plane_sum(pieces, out):
    out[...] = summed(pieces)


def finish(core, mine, theirs, image, kept, x_out, r_out, d_out):
    first = core[0] == 0
    mine, theirs = mine[...], theirs[...]
    total = jnp.concatenate(
        [jnp.where(first, mine, theirs), jnp.where(first, theirs, mine)], axis=0
    )
    cross, both = total[:Q, :Q], total[:Q, Q:]
    below, at = lower((Q, Q)), diagonal((Q, Q))
    under = jnp.where(below, both, 0.0)
    over = both - under
    matrix = jnp.where(at, total[DIAG : DIAG + 1, :Q], under + under.T)
    square = over + jnp.where(below, over.T, 0.0)
    res = restored(total[GRAM:])
    direction = kept[DIR : DIR + Q]
    step, inverse = eliminate(
        jnp.concatenate([matrix, res], axis=1),
        jnp.concatenate([res, at.astype(jnp.float32)], axis=1),
    )
    x_out[...] = kept[ITER : ITER + Q] + dot(step, direction, 0, 0)
    new_res = kept[RES : RES + Q] - dot(step, image[...], 0, 0)
    r_out[...] = new_res
    new_gram = res - dot(cross, step, 0, 0) + dot(step, dot(square, step) - cross, 0, 0)
    d_out[...] = new_res + dot(dot(inverse, new_gram), direction, 0, 0)


def swapped(value):
    return lax.ppermute(value, "core", [(0, 1), (1, 0)])


def across(value, k):
    return lax.ppermute(value, "z", [(i, i ^ k) for i in range(4)])


def exchanged(value, axes):
    return lax.all_to_all(value, axes, 0, 0, tiled=True)


def on_device(points, lengthscales, noise_level, iterate, residual, direction):
    own, cols, kept = call(
        prep,
        [f32(ROWS, 128), f32(R, COLS, 128), f32(3 * Q, 128)],
        [
            [pltpu.VMEM((N, F), jnp.float32), pltpu.VMEM((1, F), jnp.float32)],
            pltpu.SemaphoreType.DMA((5,)),
        ],
        room=ROOM,
        ins=[HBM] * 5,
    )(
        points,
        lengthscales.reshape(1, F),
        iterate.T,
        residual.T,
        direction.T,
    )
    cols = exchanged(cols, PLANE)
    rows = [own] + [across(own, k) for k in range(1, Z)]
    left, halves, sides, res_gram = call(
        spread_rows,
        [
            jax.ShapeDtypeStruct((Z * N, 6 * F), jnp.bfloat16),
            f32(Z * N, CHUNK),
            f32(2 * Q, Z * N),
            f32(SUMS - GRAM, 128),
        ],
        flops=10**8,
    )(*rows)
    other = swapped(cols)
    part = call(products_first, f32(Z * N, 2 * Q), (), 4 * 10**9, 24)(left, halves, cols)
    up, down = call(products_last, [f32(Z * H, 128)] * 2, (), 4 * 10**9, 24)(
        left, halves, other, part
    )
    up, down = call(half_way, [f32(Z * H, 128)] * 2)(up, across(up, 1), down, across(down, 3))
    got = [up, across(up, 3), down, across(down, 1)]
    image, sums = call(grams, [f32(Q, N), f32(SUMS, 128)])(
        *got, sides, res_gram, noise_level.reshape(1, 1)
    )
    core = lax.axis_index("core").reshape(1)
    both = call(pair_sum, f32(R, SUMS // 2, 128), ins=[SMEM, VM, VM])(core, sums, swapped(sums))
    half = call(plane_sum, f32(SUMS // 2, 128))(exchanged(both, PLANE))
    outs = call(finish, [f32(Q, N)] * 3, ins=[SMEM] + [VM] * 4)(
        core, half, swapped(half), image, kept
    )
    return tuple(o.T for o in outs)


def solution(mesh):
    fine = Mesh(mesh.devices.reshape(4, 2, 4, 2, 2), AXES)
    split_rows = P(AXES, None)
    return jax.shard_map(
        on_device,
        mesh=fine,
        in_specs=(split_rows, P(), P(), split_rows, split_rows, split_rows),
        out_specs=(split_rows,) * 3,
        check_vma=False,
    )
```

```python
import math

import jax
import jax.numpy as jnp
from jax import lax
from jax.experimental import pallas as pl
from jax.experimental.pallas import tpu as pltpu
from jax.sharding import Mesh, PartitionSpec as P

AXES = ("y", "xl", "z", "xh", "core")
PLANE = ("y", "xl", "xh")
N = 128
F = 128
Q = 64
R = 16
Z = 4
CHUNK = 256
H = Q // 2
HI = lax.Precision.HIGHEST
ROOT = math.sqrt(math.log2(math.e))
DIRS = N + Q
COLS = DIRS + 8
ROWS = DIRS + Q
ITER, RES, DIR = 0, Q, 2 * Q
DIAG, GRAM, SUMS = Q, Q + 8, Q + 32
SMEM = pl.BlockSpec(memory_space=pltpu.SMEM)
HBM = pl.BlockSpec(memory_space=pltpu.MemorySpace.HBM)
ROOM = 62
VM = pl.BlockSpec(memory_space=pltpu.VMEM)


def call(body, outs, scratch=(), flops=10**6, room=4, ins=None):
    return pl.pallas_call(
        body,
        out_shape=outs,
        **({} if ins is None else {"in_specs": ins}),
        out_specs=jax.tree.map(lambda _: VM, outs),
        scratch_shapes=list(scratch),
        compiler_params=pltpu.CompilerParams(vmem_limit_bytes=room * 2**20),
        cost_estimate=pl.CostEstimate(flops=flops, bytes_accessed=10**6, transcendentals=0),
    )


def f32(*shape):
    return jax.ShapeDtypeStruct(shape, jnp.float32)


def dot(a, b, ca=1, cb=0, precision=HI):
    return lax.dot_general(
        a, b, (((ca,), (cb,)), ((), ())), precision=precision, preferred_element_type=jnp.float32
    )


def low_lanes(shape):
    return lax.broadcasted_iota(jnp.int32, shape, 1) < Q


def fold(wide):
    half = wide.shape[0] // 2
    return jnp.where(low_lanes((half, 128)), wide[:half], wide[half:])


def unfold(packed):
    return jnp.concatenate([packed[:, :Q], packed[:, Q:]], axis=0)


def prep(points, scales, iterate, residual, direction, rows, cols, kept, place, sems):
    points_in, scales_in = place
    copies = [
        pltpu.make_async_copy(points, points_in, sems.at[0]),
        pltpu.make_async_copy(scales, scales_in, sems.at[1]),
        pltpu.make_async_copy(residual, kept.at[RES : RES + Q], sems.at[2]),
        pltpu.make_async_copy(direction, kept.at[DIR : DIR + Q], sems.at[3]),
        pltpu.make_async_copy(iterate, kept.at[ITER : ITER + Q], sems.at[4]),
    ]
    for copy in copies:
        copy.start()
    for copy in copies[:2]:
        copy.wait()
    unit = points_in[...] / scales_in[...] * ROOT
    half = 0.5 * jnp.sum(unit * unit, axis=1, keepdims=True)
    as_row = jnp.broadcast_to(half, (N, N)).T[:8]
    for copy in copies[2:]:
        copy.wait()
    for i in range(R):
        cols[i, :N] = unit
        cols[i, N:DIRS] = kept[DIR : DIR + Q]
        cols[i, DIRS:] = as_row
    rows[:N] = unit
    rows[N:DIRS] = kept[DIR : DIR + Q]
    rows[DIRS:] = kept[RES : RES + Q]


def split(value):
    top = value.astype(jnp.bfloat16)
    rest = value - top.astype(jnp.float32)
    mid = rest.astype(jnp.bfloat16)
    low = (rest - mid.astype(jnp.float32)).astype(jnp.bfloat16)
    return top, mid, low


def halved(residual):
    wide = dot(residual, jnp.concatenate([residual, residual], axis=0), 1, 1)
    corner = dot(residual[H:], jnp.concatenate([residual[H:]] * 4, axis=0), 1, 1)
    group = lax.broadcasted_iota(jnp.int32, (8, 128), 1) // H
    last = corner[:8]
    for g in range(1, 4):
        last = jnp.where(group == g, corner[8 * g : 8 * g + 8], last)
    return jnp.concatenate([fold(wide[:H]), last], axis=0)


def restored(packed):
    top = unfold(packed[:16])
    corner = jnp.concatenate([packed[16:, H * g : H * (g + 1)] for g in range(4)], axis=0)
    under = jnp.concatenate([jnp.zeros((H, H), jnp.float32), corner], axis=1)
    full = jnp.concatenate([top, under], axis=0)
    row = lax.broadcasted_iota(jnp.int32, (Q, Q), 0)
    column = lax.broadcasted_iota(jnp.int32, (Q, Q), 1)
    return jnp.where((row >= H) & (column < H), full.T, full)


def spread_rows(a, b, c, d, left, halves, side, gram):
    for k, rows in enumerate((a, b, c, d)):
        at = slice(k * N, (k + 1) * N)
        unit = rows[:N]
        top, mid, low = split(unit)
        left[at] = jnp.concatenate([top, top, mid, top, low, mid], axis=1)
        half = 0.5 * jnp.sum(unit * unit, axis=1, keepdims=True)
        halves[at] = jnp.broadcast_to(half, (N, CHUNK))
        side[:, at] = rows[N:]
    residual = side[Q:]
    gram[...] = halved(residual)


def partial(left, own, cols, total):
    per = CHUNK // N
    for j in range(R // per):
        blocks = [cols[j * per + i] for i in range(per)]
        tops = [split(b[:N]) for b in blocks]
        right = jnp.concatenate(
            [jnp.concatenate([t, m, t, w, t, m], axis=1) for t, m, w in tops], axis=0
        )
        pairs = [split(b[N:DIRS]) for b in blocks]
        dirs = jnp.concatenate([jnp.concatenate(p[:2], axis=0) for p in pairs], axis=1)
        half = jnp.concatenate([b[DIRS : DIRS + 1] for b in blocks], axis=1)
        inner = dot(left[...], right, 1, 1, None)
        kernel = jnp.exp2(inner - own[...] - half)
        high = kernel.astype(jnp.bfloat16)
        rest = (kernel - high.astype(jnp.float32)).astype(jnp.bfloat16)
        weights = jnp.concatenate([dirs, dirs], axis=1)
        total += dot(jnp.concatenate([high, rest], axis=1), weights, 1, 1, None)
    return total


def products_first(left, own, cols, out):
    out[...] = partial(left, own, cols, jnp.zeros((Z * N, 2 * Q), jnp.float32))


def products_last(left, own, cols, before, out):
    total = partial(left, own, cols, before[...])
    total += pltpu.roll(total, Q, 1)
    for k in range(Z):
        out[k * Q : (k + 1) * Q] = fold(total[k * N : (k + 1) * N])


def met(mine, theirs, place):
    return [
        mine[k * Q : (k + 1) * Q] + theirs[(k ^ place) * Q : ((k ^ place) + 1) * Q]
        for k in range(Z)
    ]


def half_way(mine, theirs, out):
    out[...] = jnp.concatenate(met(mine, theirs, 1), axis=0)


def summed(pieces):
    total = pieces[0]
    for j in range(1, pieces.shape[0]):
        total += pieces[j]
    return total


def lower(shape):
    return lax.broadcasted_iota(jnp.int32, shape, 0) > lax.broadcasted_iota(jnp.int32, shape, 1)


def diagonal(shape):
    return lax.broadcasted_iota(jnp.int32, shape, 0) == lax.broadcasted_iota(jnp.int32, shape, 1)


def grams(mine, theirs, sides, res_gram, noise, image_out, sums):
    parts = []
    for block in met(mine, theirs, 2):
        turned = block.T
        parts += [turned[:Q], turned[Q:]]
    direction = sides[:Q]
    image = jnp.concatenate(parts, axis=1) + noise[0, 0] * direction
    image_out[...] = image[:, :N]
    wide = dot(image, jnp.concatenate([sides[...], image], axis=0), 1, 1)
    gram = 0.5 * (wide[:, :Q] + dot(direction, image, 1, 1))
    cross, square = wide[:, Q : 2 * Q], wide[:, 2 * Q :]
    both = jnp.where(lower((Q, Q)), gram, square)
    sums[:Q] = jnp.concatenate([cross, both], axis=1)
    along = jnp.sum(jnp.where(diagonal((Q, Q)), gram, 0.0), axis=0, keepdims=True)
    sums[DIAG:GRAM] = jnp.broadcast_to(jnp.concatenate([along, along], axis=1), (8, 128))
    sums[GRAM:] = res_gram[...]


def eliminate(*matrices):
    sub = lax.broadcasted_iota(jnp.int32, (8, 128), 0)
    each = range(len(matrices))
    slabs = [[m[8 * r : 8 * r + 8] for r in range(8)] for m in matrices]
    for k in range(8):
        spread = [
            [
                [
                    jnp.broadcast_to(slabs[m][r][:, 8 * k + j : 8 * k + j + 1], (8, 128))
                    for j in range(8)
                ]
                for r in range(8)
            ]
            for m in each
        ]
        own = [spread[m][k] for m in each]
        pivot = [slabs[m][k] for m in each]
        for j in range(8):
            inverse = [1.0 / jnp.broadcast_to(own[m][j][j : j + 1], (8, 128)) for m in each]

            def cleared(value, m):
                row = jnp.broadcast_to(value[j : j + 1], (8, 128)) * inverse[m]
                return jnp.where(sub == j, row, value - own[m][j] * row)

            pivot = [cleared(pivot[m], m) for m in each]
            own = [own[m][: j + 1] + [cleared(c, m) for c in own[m][j + 1 :]] for m in each]
        for r in range(8):
            if r != k:
                for j in range(8):
                    for m in each:
                        slabs[m][r] = slabs[m][r] - spread[m][r][j] * jnp.broadcast_to(
                            pivot[m][j : j + 1], (8, 128)
                        )
        for m in each:
            slabs[m][k] = pivot[m]
    return [jnp.concatenate(rows, axis=0)[:, Q:] for rows in slabs]


def half_of(core, total):
    return jnp.where(core[0] == 0, total[: SUMS // 2], total[SUMS // 2 :])


def pair_sum(core, a, b, out):
    total = half_of(core, a[...] + b[...])
    for j in range(R):
        out[j] = total


def plane_sum(pieces, out):
    out[...] = summed(pieces)


def finish(core, mine, theirs, image, kept, x_out, r_out, d_out):
    first = core[0] == 0
    mine, theirs = mine[...], theirs[...]
    total = jnp.concatenate(
        [jnp.where(first, mine, theirs), jnp.where(first, theirs, mine)], axis=0
    )
    cross, both = total[:Q, :Q], total[:Q, Q:]
    below, at = lower((Q, Q)), diagonal((Q, Q))
    under = jnp.where(below, both, 0.0)
    over = both - under
    matrix = jnp.where(at, total[DIAG : DIAG + 1, :Q], under + under.T)
    square = over + jnp.where(below, over.T, 0.0)
    res = restored(total[GRAM:])
    direction = kept[DIR : DIR + Q]
    step, inverse = eliminate(
        jnp.concatenate([matrix, res], axis=1),
        jnp.concatenate([res, at.astype(jnp.float32)], axis=1),
    )
    x_out[...] = kept[ITER : ITER + Q] + dot(step, direction, 0, 0)
    new_res = kept[RES : RES + Q] - dot(step, image[...], 0, 0)
    r_out[...] = new_res
    new_gram = res - dot(cross, step, 0, 0) + dot(step, dot(square, step) - cross, 0, 0)
    d_out[...] = new_res + dot(new_gram, dot(inverse, direction, 1, 0), 0, 0)


def swapped(value):
    return lax.ppermute(value, "core", [(0, 1), (1, 0)])


def across(value, k):
    return lax.ppermute(value, "z", [(i, i ^ k) for i in range(4)])


def exchanged(value, axes):
    return lax.all_to_all(value, axes, 0, 0, tiled=True)


def on_device(points, lengthscales, noise_level, iterate, residual, direction):
    own, cols, kept = call(
        prep,
        [f32(ROWS, 128), f32(R, COLS, 128), f32(3 * Q, 128)],
        [
            [pltpu.VMEM((N, F), jnp.float32), pltpu.VMEM((1, F), jnp.float32)],
            pltpu.SemaphoreType.DMA((5,)),
        ],
        room=ROOM,
        ins=[HBM] * 5,
    )(
        points,
        lengthscales.reshape(1, F),
        iterate.T,
        residual.T,
        direction.T,
    )
    cols = exchanged(cols, PLANE)
    rows = [own] + [across(own, k) for k in range(1, Z)]
    left, halves, sides, res_gram = call(
        spread_rows,
        [
            jax.ShapeDtypeStruct((Z * N, 6 * F), jnp.bfloat16),
            f32(Z * N, CHUNK),
            f32(2 * Q, Z * N),
            f32(SUMS - GRAM, 128),
        ],
        flops=10**8,
    )(*rows)
    other = swapped(cols)
    part = call(products_first, f32(Z * N, 2 * Q), (), 4 * 10**9, 24)(left, halves, cols)
    sent = call(products_last, f32(Z * Q, 128), (), 4 * 10**9, 24)(
        left, halves, other, part
    )
    sent = call(half_way, f32(Z * Q, 128))(sent, across(sent, 1))
    got = [sent, across(sent, 2)]
    image, sums = call(grams, [f32(Q, N), f32(SUMS, 128)])(
        *got, sides, res_gram, noise_level.reshape(1, 1)
    )
    core = lax.axis_index("core").reshape(1)
    both = call(pair_sum, f32(R, SUMS // 2, 128), ins=[SMEM, VM, VM])(core, sums, swapped(sums))
    half = call(plane_sum, f32(SUMS // 2, 128))(exchanged(both, PLANE))
    outs = call(finish, [f32(Q, N)] * 3, ins=[SMEM] + [VM] * 4)(
        core, half, swapped(half), image, kept
    )
    return tuple(o.T for o in outs)


def solution(mesh):
    fine = Mesh(mesh.devices.reshape(4, 2, 4, 2, 2), AXES)
    split_rows = P(AXES, None)
    return jax.shard_map(
        on_device,
        mesh=fine,
        in_specs=(split_rows, P(), P(), split_rows, split_rows, split_rows),
        out_specs=(split_rows,) * 3,
        check_vma=False,
    )
```
